128 devices in a mesh: section: 8 (over y, core), row: 16 (over z, x).
Axes of the slice: x: 4, y: 4, z: 4, core: 2. Of those that a mesh axis runs over, the one named last changes fastest.
Arguments:
- diag_blocks: float32 [8, 2, 16, 256, 256], P('section', None, 'row'), may hold values from -9 to 9, as said below
- coupling_blocks: float32 [8, 2, 16, 256, 256], P('section', None, 'row'), as said below
Outputs:
- reduced_diag: float32 [8, 2, 16, 256, 256], P('section', None, 'row')
- reduced_coupling: float32 [8, 2, 16, 256, 256], P('section', None, 'row')
The draws below stay inside these ranges and needn't reach their ends.
Inputs may be any that keep to these rules, and one draw needn't show every extreme that they name: `diag_blocks`: every block is symmetric. `coupling_blocks`: every block is three times the identity plus a random part whose entries are at most 5 / sqrt(256) in magnitude and whose spectral norm is at most 2.5, so every block is invertible.
All inputs are finite; a program needn't handle non-finite values.
Results may differ from the reference program's by a relative error of at most 0.0003.
Values sent between devices are 32-bit elements; how exact they have to be, the bound alone decides.
No kernel may reach another device: no remote copies, remote signals or barrier semaphores. Data moves between devices by JAX's collectives and lax.ppermute only.
A program may use at most 64 MiB of HBM per device.

```python
import jax
import jax.numpy as jnp
from jax import lax

D = 256
MB = 2
NBLK = 16
GROUPS = 8


def draw_diag_blocks(key, part):
    full_shape = (GROUPS, MB, NBLK, D, D)
    random_part = jnp.clip(jax.random.normal(key, full_shape, jnp.float32), -6.0, 6.0)
    return (random_part + jnp.swapaxes(random_part, -1, -2)) * 0.7071


def draw_coupling_blocks(key, part):
    full_shape = (GROUPS, MB, NBLK, D, D)
    random_part = jnp.clip(jax.random.normal(key, full_shape, jnp.float32), -5.0, 5.0)
    identity = jnp.eye(D, dtype=jnp.float32)
    return 3.0 * identity + random_part / jnp.sqrt(jnp.float32(D))


def setup_inputs(seed: int = 0) -> dict:
    arg_keys = jax.random.split(jax.random.key(seed), 3)
    return {
        "diag_blocks": draw_diag_blocks(jax.random.fold_in(arg_keys[2], 71), 0),
        "coupling_blocks": draw_coupling_blocks(jax.random.fold_in(arg_keys[2], 71), 0),
    }


highest = lax.Precision.HIGHEST

def product(left, right):
    return jnp.dot(left.astype(jnp.float32), right.astype(jnp.float32), precision=highest, preferred_element_type=jnp.float32)

def qfactor(panel_now):
    gram_first = product(panel_now.T, panel_now)
    lower_first = jnp.linalg.cholesky(gram_first)
    first_pass = jax.scipy.linalg.solve_triangular(lower_first, panel_now.T, lower=True).T
    gram_second = product(first_pass.T, first_pass)
    lower_second = jnp.linalg.cholesky(gram_second)
    orthogonal = jax.scipy.linalg.solve_triangular(lower_second, first_pass.T, lower=True).T
    upper_part = product(lower_second.T, lower_first.T)
    return (orthogonal, upper_part)

def sweep_matrix(diagonal, coupling):
    identity = jnp.eye(D, dtype=jnp.float32)

    def sweep_step(previous, blocks_pair):
        diag_now, coupling_now = blocks_pair
        panel_now = product(coupling_now, previous)
        orthogonal, upper_part = qfactor(panel_now)
        new_diag = product(product(orthogonal.T, diag_now), orthogonal)
        return (orthogonal, (new_diag, upper_part))
    unused, outputs = lax.scan(sweep_step, identity, (diagonal, coupling))
    return outputs

def reference(diag_blocks, coupling_blocks):
    flat_diag = diag_blocks.reshape(GROUPS * MB, NBLK, D, D)
    flat_coupling = coupling_blocks.reshape(GROUPS * MB, NBLK, D, D)
    new_diag, triangles = jax.vmap(sweep_matrix)(flat_diag, flat_coupling)
    new_diag = new_diag.reshape(GROUPS, MB, NBLK, D, D)
    triangles = triangles.reshape(GROUPS, MB, NBLK, D, D)
    return (new_diag, triangles)
```

```python
import functools

import jax
import jax.numpy as jnp
from jax import lax
from jax.experimental import pallas as pl
from jax.experimental.pallas import tpu as pltpu
from jax.sharding import PartitionSpec as P

D = 256
B = 16
HALF = 128
F32 = jnp.float32
BF16 = jnp.bfloat16
KAPPA2 = 2.0e8


def dg(a, b, ca, cb):
    return lax.dot_general(a, b, (((ca,), (cb,)), ((), ())), preferred_element_type=F32)


def split2(x):
    h = x.astype(BF16)
    return h, (x - h.astype(F32)).astype(BF16)


def split3(x):
    h = x.astype(BF16)
    r = x - h.astype(F32)
    m = r.astype(BF16)
    return h, m, (r - m.astype(F32)).astype(BF16)


def mm(a, b, ca=1, cb=0, passes=6):
    if passes == 3:
        ah, al = split2(a)
        bh, bl = split2(b)
        return dg(al, bh, ca, cb) + dg(ah, bl, ca, cb) + dg(ah, bh, ca, cb)
    ah, am, al = split3(a)
    bh, bm, bl = split3(b)
    small = dg(al, bh, ca, cb) + dg(ah, bl, ca, cb) + dg(am, bm, ca, cb)
    return (small + (dg(am, bh, ca, cb) + dg(ah, bm, ca, cb))) + dg(ah, bh, ca, cb)


def square_iota():
    return (
        lax.broadcasted_iota(jnp.int32, (D, D), 0),
        lax.broadcasted_iota(jnp.int32, (D, D), 1),
    )


def chol_inv(a_ref, nb):
    row = lax.broadcasted_iota(jnp.int32, (B, HALF), 0)
    lane2 = lax.broadcasted_iota(jnp.int32, (B, D), 1)
    row2 = lax.broadcasted_iota(jnp.int32, (B, D), 0)
    for p in range(D // B):
        k = p * B
        for m in range(nb):
            s = a_ref[m, k : k + B, :]
            cols = [jnp.broadcast_to(s[:, k + c : k + c + 1], (B, HALF)) for c in range(B)]
            own = (lane2 >= k) & (lane2 < k + B)
            s = jnp.where(own, jnp.where(lane2 - k == row2, 1.0, 0.0), s)
            sa, sb = s[:, :HALF], s[:, HALF:]
            pivots = jnp.ones((B, HALF), F32)
            for r in range(B):
                piv = jnp.broadcast_to(cols[r][r : r + 1, :], (B, HALF))
                l = jnp.where(row > r, cols[r] * (1.0 / piv), 0.0)
                pivots = jnp.where(row == r, piv, pivots)
                for c in range(r + 1, B):
                    cols[c] = cols[c] - l * jnp.broadcast_to(cols[c][r : r + 1, :], (B, HALF))
                sa = sa - l * jnp.broadcast_to(sa[r : r + 1, :], (B, HALF))
                sb = sb - l * jnp.broadcast_to(sb[r : r + 1, :], (B, HALF))
            rs = lax.rsqrt(pivots)
            s = jnp.concatenate([sa * rs, sb * rs], 1)
            a_ref[m, k : k + B, :] = s
            if k + B < D:
                n0 = HALF if k + B >= HALF else 0
                h, md, lo = split3(s)
                left = jnp.concatenate([lo, h, md, md, h, h], 0)
                right = jnp.concatenate([h, lo, md, h, md, h], 0)
                u = dg(left[:, n0:], right, 0, 0)
                tail = a_ref[m, k + B :, :]
                lt = lax.broadcasted_iota(jnp.int32, (D - k - B, D), 1)
                kept = jnp.where((lt >= k) & (lt < k + B), 0.0, tail)
                a_ref[m, k + B :, :] = kept - u[k + B - n0 :, :]


def window_kernel(pos_ref, r0, r1, r2, r3, prev_ref, t_ref, blk):
    x = pos_ref[1]
    mine = pos_ref[2]
    r, c = square_iota()
    for s, ref in enumerate((r0, r1, r2, r3)):
        blk[lax.rem(x - s + 4, 4)] = ref[...]
    for m in range(2):
        p0 = blk[0, m]
        p1 = mm(blk[1, m], p0)
        p2 = mm(blk[2, m], p1)

        @pl.when(x == 0)
        def _():
            prev_ref[m] = jnp.where(r == c, 1.0, 0.0)

        @pl.when(x == 1)
        def _():
            prev_ref[m] = p0

        @pl.when(x == 2)
        def _():
            prev_ref[m] = p1

        @pl.when(x == 3)
        def _():
            prev_ref[m] = p2

        @pl.when(mine == m)
        def _():
            t_ref[...] = mm(blk[3, m], p2)


def slice_kernel(pos_ref, t1, t2, t3, e_ref):
    z = pos_ref[0]
    half = pos_ref[3]
    r = lax.broadcasted_iota(jnp.int32, (D, HALF), 0)
    c = lax.broadcasted_iota(jnp.int32, (D, HALF), 1)
    e_ref[...] = jnp.where(r == c + half * HALF, 1.0, 0.0)

    @pl.when(z >= 3)
    def _():
        e_ref[...] = mm(t3[...], e_ref[...])

    @pl.when(z >= 2)
    def _():
        e_ref[...] = mm(t2[...], e_ref[...])

    @pl.when(z >= 1)
    def _():
        e_ref[...] = mm(t1[...], e_ref[...])


def factor_kernel(pos_ref, prev_ref, e0, e1, e2, e3, c_ref, m_ref, x_ref, stat_ref, e_all):
    x = pos_ref[1]
    for s, ref in enumerate((e0, e1, e2, e3)):
        e_all[lax.rem(x - s + 4, 4)] = ref[...]
    for m, (lo, hi) in enumerate(((1, 2), (0, 3))):
        entry = jnp.concatenate([e_all[lo], e_all[hi]], 1)
        before = mm(prev_ref[m], entry)
        m_ref[m] = before
        m_ref[2 + m] = mm(c_ref[m], before)
    for m in range(4):
        full = m_ref[m]
        x_ref[m] = mm(full, full, 0, 0)
    chol_inv(x_ref, 4)
    r, c = square_iota()
    worst = jnp.zeros((8, HALF), F32)
    for m in range(4):
        inv = jnp.where(c <= r, x_ref[m], 0.0)
        full = m_ref[m]
        x_ref[m] = inv
        size = jnp.sum(jnp.sum(inv * inv, axis=0, keepdims=True), axis=1, keepdims=True)
        size = size * jnp.sum(jnp.sum(full * full, axis=0, keepdims=True), axis=1, keepdims=True)
        worst = jnp.maximum(worst, jnp.broadcast_to(jnp.where(size < KAPPA2, 0.0, 1.0), (8, HALF)))
    stat_ref[...] = worst


def finish_kernel(m_ref, x_ref, c_ref, d_ref, n_ref, r_ref, q_ref, y_ref):
    r, c = square_iota()
    for m in range(4):
        y = mm(m_ref[m], x_ref[m], 1, 1)
        err = mm(y, y, 0, 0, passes=3) - jnp.where(r == c, 1.0, 0.0)
        upper = jnp.where(c > r, err, jnp.where(c == r, 0.5 * err, 0.0))
        y_ref[m] = y - mm(y, upper, passes=3)
    for m in range(2):
        before = y_ref[m]
        q = y_ref[2 + m]
        q_ref[m] = q
        r_ref[m] = jnp.where(c >= r, mm(q, mm(c_ref[m], before), 0, 0), 0.0)
        n_ref[m] = mm(mm(q, d_ref[m], 0, 0), q)


def struct(*shape):
    return jax.ShapeDtypeStruct(shape, F32)


def call(kernel, outs, scratch, name):
    def run(*args):
        smem = name != "finish"
        specs = [pl.BlockSpec(memory_space=pltpu.VMEM)] * len(args)
        if smem:
            specs[0] = pl.BlockSpec(memory_space=pltpu.SMEM)
        return pl.pallas_call(
            kernel,
            out_shape=outs,
            in_specs=specs,
            out_specs=jax.tree.map(lambda _: pl.BlockSpec(memory_space=pltpu.VMEM), outs),
            scratch_shapes=scratch,
            compiler_params=pltpu.CompilerParams(vmem_limit_bytes=48 * 2**20),
            name=name,
        )(*args)

    return run


window = call(
    window_kernel, (struct(2, D, D), struct(D, D)), [pltpu.VMEM((4, 2, D, D), F32)], "window"
)
column_slice = call(slice_kernel, struct(D, HALF), [], "column_slice")
factor = call(
    factor_kernel,
    (struct(4, D, D), struct(4, D, D), struct(8, HALF)),
    [pltpu.VMEM((4, D, HALF), F32)],
    "factor",
)
finish = call(
    finish_kernel,
    (struct(2, D, D), struct(2, D, D), struct(2, D, D)),
    [pltpu.VMEM((4, D, D), F32)],
    "finish",
)


def x_shift(value, s):
    return lax.ppermute(value, "row", [(i, (i // 4) * 4 + (i + s) % 4) for i in range(16)])


def z_shift(value, s):
    return lax.ppermute(value, "row", [(i, i + 4 * s) for i in range(16 - 4 * s)])


def z_ring(value, s):
    return lax.ppermute(value, "row", [(i, (i + 4 * s) % 16) for i in range(16)])


def any_in_row(flag):
    for move in (x_shift, z_ring):
        flag = functools.reduce(jnp.maximum, [move(flag, s) for s in (1, 2, 3)], flag)
    return flag


def sequential(pos, coupling, diagonal):
    position = lax.axis_index("row")
    x = position % 4
    eye = jnp.eye(D, dtype=F32)
    halves = jnp.stack([eye[:, :HALF], eye[:, HALF:]])
    unit = [halves[jnp.where((x - s) % 4 >= 2, 1, 0)] for s in range(4)]

    def step(i, carried):
        before, new, tri = carried
        full, inv, _ = factor(pos, before, *unit, coupling)
        new_now, tri_now, q = finish(full, inv, coupling, diagonal)
        keep = i == position
        new = jnp.where(keep, new_now, new)
        tri = jnp.where(keep, tri_now, tri)
        before = lax.ppermute(q, "row", [(j, j + 1) for j in range(15)])
        return before, new, tri

    start = jnp.broadcast_to(eye, (2, D, D))
    zero = jnp.zeros((2, D, D), F32)
    _, new, tri = lax.fori_loop(0, 16, step, (start, zero, zero))
    return new, tri


def shards(diag_blocks, coupling_blocks):
    diagonal = diag_blocks.reshape(2, D, D)
    coupling = coupling_blocks.reshape(2, D, D)
    position = lax.axis_index("row")
    z, x = position // 4, position % 4
    mine = jnp.where((x == 0) | (x == 3), 1, 0)
    half = jnp.where(x >= 2, 1, 0)
    pos = jnp.stack([z, x, mine, half]).astype(jnp.int32)

    others = [x_shift(coupling, s) for s in (1, 2, 3)]
    prev, total = window(pos, coupling, *others)
    below = [z_shift(total, s) for s in (1, 2, 3)]
    part = column_slice(pos, *below)
    parts = [x_shift(part, s) for s in (1, 2, 3)]
    full, inv, stat = factor(pos, prev, part, *parts, coupling)
    bad = any_in_row(stat)
    new, tri, _ = finish(full, inv, coupling, diagonal)
    new, tri = lax.cond(
        bad[0, 0] > 0.0,
        lambda: sequential(pos, coupling, diagonal),
        lambda: (new, tri),
    )
    shape = diag_blocks.shape
    return new.reshape(shape), tri.reshape(shape)


def solution(mesh):
    placed = P("section", None, "row", None, None)
    return jax.shard_map(
        shards,
        mesh=mesh,
        in_specs=(placed, placed),
        out_specs=(placed, placed),
        check_vma=False,
    )
```

```python
import functools

import jax
import jax.numpy as jnp
from jax import lax
from jax.experimental import pallas as pl
from jax.experimental.pallas import tpu as pltpu
from jax.sharding import PartitionSpec as P

D = 256
B = 16
HALF = 128
F32 = jnp.float32
BF16 = jnp.bfloat16
KAPPA2 = 3.0e7


def dg(a, b, ca, cb):
    return lax.dot_general(a, b, (((ca,), (cb,)), ((), ())), preferred_element_type=F32)


def split2(x):
    h = x.astype(BF16)
    return h, (x - h.astype(F32)).astype(BF16)


def split3(x):
    h = x.astype(BF16)
    r = x - h.astype(F32)
    m = r.astype(BF16)
    return h, m, (r - m.astype(F32)).astype(BF16)


def mm(a, b, ca=1, cb=0, passes=6):
    if passes == 3:
        ah, al = split2(a)
        bh, bl = split2(b)
        return dg(al, bh, ca, cb) + dg(ah, bl, ca, cb) + dg(ah, bh, ca, cb)
    ah, am, al = split3(a)
    bh, bm, bl = split3(b)
    small = dg(al, bh, ca, cb) + dg(ah, bl, ca, cb) + dg(am, bm, ca, cb)
    return (small + (dg(am, bh, ca, cb) + dg(ah, bm, ca, cb))) + dg(ah, bh, ca, cb)


def square_iota():
    return (
        lax.broadcasted_iota(jnp.int32, (D, D), 0),
        lax.broadcasted_iota(jnp.int32, (D, D), 1),
    )


def chol_inv(a_ref, nb):
    row = lax.broadcasted_iota(jnp.int32, (B, HALF), 0)
    lane2 = lax.broadcasted_iota(jnp.int32, (B, D), 1)
    row2 = lax.broadcasted_iota(jnp.int32, (B, D), 0)
    for p in range(D // B):
        k = p * B
        for m in range(nb):
            s = a_ref[m, k : k + B, :]
            cols = [jnp.broadcast_to(s[:, k + c : k + c + 1], (B, HALF)) for c in range(B)]
            own = (lane2 >= k) & (lane2 < k + B)
            s = jnp.where(own, jnp.where(lane2 - k == row2, 1.0, 0.0), s)
            sa, sb = s[:, :HALF], s[:, HALF:]
            pivots = jnp.ones((B, HALF), F32)
            for r in range(B):
                piv = jnp.broadcast_to(cols[r][r : r + 1, :], (B, HALF))
                l = jnp.where(row > r, cols[r] * (1.0 / piv), 0.0)
                pivots = jnp.where(row == r, piv, pivots)
                for c in range(r + 1, B):
                    cols[c] = cols[c] - l * jnp.broadcast_to(cols[c][r : r + 1, :], (B, HALF))
                sa = sa - l * jnp.broadcast_to(sa[r : r + 1, :], (B, HALF))
                sb = sb - l * jnp.broadcast_to(sb[r : r + 1, :], (B, HALF))
            rs = lax.rsqrt(pivots)
            s = jnp.concatenate([sa * rs, sb * rs], 1)
            a_ref[m, k : k + B, :] = s
            if k + B < D:
                n0 = HALF if k + B >= HALF else 0
                h, md, lo = split3(s)
                left = jnp.concatenate([lo, h, md, md, h, h], 0)
                right = jnp.concatenate([h, lo, md, h, md, h], 0)
                u = dg(left[:, n0:], right, 0, 0)
                tail = a_ref[m, k + B :, :]
                lt = lax.broadcasted_iota(jnp.int32, (D - k - B, D), 1)
                kept = jnp.where((lt >= k) & (lt < k + B), 0.0, tail)
                a_ref[m, k + B :, :] = kept - u[k + B - n0 :, :]


TABLE = (
    (6, 1, 3, 8, 0, 0, 2, 7, 7, 9),
    (5, 4, 0, 0, 0, 0, 1, 2, 6, 8),
    (4, 5, 3, 6, 0, 0, 2, 5, 9, 8),
    (6, 3, 1, 8, 2, 5, 3, 10, 8, 9),
)


def eye_value():
    r, c = square_iota()
    return jnp.where(r == c, 1.0, 0.0)


def pair_kernel(pos_ref, c_ref, r0, r1, w_ref, v_ref, buf):
    x = pos_ref[1]
    odd = lax.rem(x, 2)
    high = x // 2
    buf[odd] = c_ref[0]
    buf[1 - odd] = r0[...]
    buf[2 + high] = c_ref[1]
    buf[3 - high] = r1[...]
    w_ref[...] = mm(buf[1], buf[0])
    outer = (x == 0) | (x == 3)

    @pl.when(outer)
    def _():
        v_ref[...] = buf[2]

    @pl.when(jnp.logical_not(outer))
    def _():
        v_ref[...] = mm(buf[3], buf[2])


def window_kernel(tab_ref, c_ref, r0, r1, w, q0, q1, prev_ref, t_ref, buf):
    buf[0] = c_ref[0]
    buf[1] = c_ref[1]
    for k, ref in enumerate((r0, r1, w, q0, q1)):
        buf[2 + k] = ref[...]
    buf[7] = eye_value()

    def step(i, _):
        buf[8 + i] = mm(buf[tab_ref[2 * i]], buf[tab_ref[2 * i + 1]])
        return 0

    lax.fori_loop(0, tab_ref[6], step, 0)
    prev_ref[0] = buf[tab_ref[7]]
    prev_ref[1] = buf[tab_ref[8]]
    t_ref[...] = buf[tab_ref[9]]


def entry_kernel(pos_ref, t1, t2, t3, e_ref, buf):
    z = pos_ref[0]
    buf[0] = eye_value()
    for k, ref in enumerate((t1, t2, t3)):
        buf[1 + k] = ref[...]
    e_ref[...] = buf[z]

    def step(i, _):
        e_ref[...] = mm(buf[z - 1 - i], e_ref[...])
        return 0

    lax.fori_loop(0, z - 1, step, 0)


def factor_kernel(pos_ref, prev_ref, own, other, c_ref, m_ref, x_ref, stat_ref, e_all):
    mine = pos_ref[2]
    e_all[mine] = own[...]
    e_all[1 - mine] = other[...]
    for m in range(2):
        before = mm(prev_ref[m], e_all[m])
        m_ref[m] = before
        m_ref[2 + m] = mm(c_ref[m], before)
    for m in range(4):
        full = m_ref[m]
        x_ref[m] = mm(full, full, 0, 0)
    chol_inv(x_ref, 4)
    r, c = square_iota()
    worst = jnp.zeros((8, HALF), F32)
    for m in range(4):
        inv = jnp.where(c <= r, x_ref[m], 0.0)
        full = m_ref[m]
        x_ref[m] = inv
        size = jnp.sum(jnp.sum(inv * inv, axis=0, keepdims=True), axis=1, keepdims=True)
        size = size * jnp.sum(jnp.sum(full * full, axis=0, keepdims=True), axis=1, keepdims=True)
        worst = jnp.maximum(worst, jnp.broadcast_to(jnp.where(size < KAPPA2, 0.0, 1.0), (8, HALF)))
    stat_ref[...] = worst


def refined(y):
    r, c = square_iota()
    err = mm(y, y, 0, 0, passes=3) - eye_value()
    upper = jnp.where(c > r, err, jnp.where(c == r, 0.5 * err, 0.0))
    return y - mm(y, upper, passes=3)


def finish_kernel(m_ref, x_ref, c_ref, d_ref, n_ref, r_ref, y_ref):
    r, c = square_iota()
    for m in range(4):
        y_ref[m] = refined(mm(m_ref[m], x_ref[m], 1, 1))
    for m in range(2):
        before = y_ref[m]
        q = y_ref[2 + m]
        r_ref[m] = jnp.where(c >= r, mm(q, mm(c_ref[m], before), 0, 0), 0.0)
        n_ref[m] = mm(mm(q, d_ref[m], 0, 0), q)


def chain_kernel(before_ref, c_ref, d_ref, n_ref, r_ref, q_ref, a_ref):
    r, c = square_iota()
    lane = lax.broadcasted_iota(jnp.int32, (1, D), 1)

    def one(m, _):
        n_ref[m] = mm(c_ref[m], before_ref[m])
        a_ref[...] = mm(n_ref[m], n_ref[m], 0, 0)

        def column(k, _):
            a = a_ref[...]
            row = a_ref[pl.ds(k, 1), :]
            pivot = jnp.sum(jnp.where(lane == k, row, 0.0), axis=1, keepdims=True)
            rs = lax.rsqrt(pivot)
            row = jnp.where(lane == k, 1.0, row) * rs
            factor_col = jnp.sum(jnp.where(c == k, a, 0.0), axis=1, keepdims=True) * rs
            below = jnp.where(c == k, 0.0, a) - factor_col * row
            a_ref[...] = jnp.where(r > k, below, jnp.where(r == k, row, a))
            return 0

        lax.fori_loop(0, D, column, 0)
        q_ref[m] = mm(n_ref[m], jnp.where(c <= r, a_ref[...], 0.0), 1, 1)

        def again(_, carry):
            q_ref[m] = refined(q_ref[m])
            return carry

        lax.fori_loop(0, 2, again, 0)
        q = q_ref[m]
        r_ref[m] = jnp.where(c >= r, mm(q, n_ref[m], 0, 0), 0.0)
        n_ref[m] = mm(mm(q, d_ref[m], 0, 0), q)
        return 0

    lax.fori_loop(0, 2, one, 0)


def struct(*shape):
    return jax.ShapeDtypeStruct(shape, F32)


VMEM = pl.BlockSpec(memory_space=pltpu.VMEM)
SMEM = pl.BlockSpec(memory_space=pltpu.SMEM)


def call(kernel, outs, scratch, name, table=True):
    def run(*args):
        specs = [VMEM] * len(args)
        if table:
            specs[0] = SMEM
        return pl.pallas_call(
            kernel,
            out_shape=outs,
            in_specs=specs,
            out_specs=jax.tree.map(lambda _: VMEM, outs),
            scratch_shapes=[pltpu.VMEM(shape, F32) for shape in scratch],
            compiler_params=pltpu.CompilerParams(vmem_limit_bytes=48 * 2**20),
            name=name,
        )(*args)

    return run


SQUARE = struct(D, D)
TWO = struct(2, D, D)
FOUR = struct(4, D, D)
pair = call(pair_kernel, (SQUARE, SQUARE), [(4, D, D)], "pair")
window = call(window_kernel, (TWO, SQUARE), [(11, D, D)], "window")
entry = call(entry_kernel, SQUARE, [(4, D, D)], "entry")
factor = call(factor_kernel, (FOUR, FOUR, struct(8, HALF)), [(2, D, D)], "factor")
finish = call(finish_kernel, (TWO, TWO), [(4, D, D)], "finish", table=False)
chain = call(chain_kernel, (TWO, TWO, TWO), [(D, D)], "chain", table=False)


def x_move(value, to):
    return lax.ppermute(value, "row", [(i, (i // 4) * 4 + to(i % 4)) for i in range(16)])


def z_move(value, s):
    return lax.ppermute(value, "row", [(i, i + 4 * s) for i in range(16 - 4 * s)])


def z_ring(value, s):
    return lax.ppermute(value, "row", [(i, (i + 4 * s) % 16) for i in range(16)])


def x_pairs(value):
    return x_move(value, lambda x: x ^ 1)


def x_mirror(value):
    return x_move(value, lambda x: 3 - x)


def any_in_row(flag):
    moved = [x_move(flag, lambda x, s=s: (x + s) % 4) for s in (1, 2, 3)]
    flag = functools.reduce(jnp.maximum, moved, flag)
    return functools.reduce(jnp.maximum, [z_ring(flag, s) for s in (1, 2, 3)], flag)


def shards(diag_blocks, coupling_blocks):
    diagonal = diag_blocks.reshape(2, D, D)
    coupling = coupling_blocks.reshape(2, D, D)
    position = lax.axis_index("row")
    z, x = position // 4, position % 4
    mine = jnp.where((x == 0) | (x == 3), 1, 0)
    pos = jnp.stack([z, x, mine]).astype(jnp.int32)
    table = jnp.asarray(TABLE, jnp.int32)[x]

    r0, r1 = x_pairs(coupling[0]), x_mirror(coupling[1])
    w, v = pair(pos, coupling, r0, r1)
    q0, q1 = x_mirror(w), x_pairs(v)
    prev, total = window(table, coupling, r0, r1, w, q0, q1)
    below = [z_move(total, s) for s in (1, 2, 3)]
    own = entry(pos, *below)
    full, inv, stat = factor(pos, prev, own, x_pairs(own), coupling)
    bad = any_in_row(stat)
    new, tri = finish(full, inv, coupling, diagonal)

    def step(i, carried):
        before, new, tri = carried
        new_now, tri_now, q = chain(before, coupling, diagonal)
        keep = i == position
        new = jnp.where(keep, new_now, new)
        tri = jnp.where(keep, tri_now, tri)
        return lax.ppermute(q, "row", [(j, j + 1) for j in range(15)]), new, tri

    rounds = jnp.where(bad[0, 0] > 0.0, 16, 0)
    eyes = jnp.broadcast_to(jnp.eye(D, dtype=F32), (2, D, D))
    _, new, tri = lax.fori_loop(0, rounds, step, (eyes, new, tri))
    shape = diag_blocks.shape
    return new.reshape(shape), tri.reshape(shape)


def solution(mesh):
    placed = P("section", None, "row", None, None)
    return jax.shard_map(
        shards,
        mesh=mesh,
        in_specs=(placed, placed),
        out_specs=(placed, placed),
        check_vma=False,
    )
```

```python
import functools

import jax
import jax.numpy as jnp
from jax import lax
from jax.experimental import pallas as pl
from jax.experimental.pallas import tpu as pltpu
from jax.sharding import PartitionSpec as P

D = 256
B = 16
HALF = 128
SOLVE = 3
GRAM = 6
F32 = jnp.float32
BF16 = jnp.bfloat16
LIMIT = 17.97
ORTHO2 = 4.0e-4


def dg(a, b, ca, cb):
    return lax.dot_general(a, b, (((ca,), (cb,)), ((), ())), preferred_element_type=F32)


def split2(x):
    h = x.astype(BF16)
    return h, (x - h.astype(F32)).astype(BF16)


def split3(x):
    h = x.astype(BF16)
    r = x - h.astype(F32)
    m = r.astype(BF16)
    return h, m, (r - m.astype(F32)).astype(BF16)


def mm(a, b, ca=1, cb=0, passes=6):
    if passes == 1:
        return dg(a.astype(BF16), b.astype(BF16), ca, cb)
    if passes == 3:
        ah, al = split2(a)
        bh, bl = split2(b)
        return dg(al, bh, ca, cb) + dg(ah, bl, ca, cb) + dg(ah, bh, ca, cb)
    ah, am, al = split3(a)
    bh, bm, bl = split3(b)
    small = dg(al, bh, ca, cb) + dg(ah, bl, ca, cb) + dg(am, bm, ca, cb)
    return (small + (dg(am, bh, ca, cb) + dg(ah, bm, ca, cb))) + dg(ah, bh, ca, cb)


def square_iota():
    return (
        lax.broadcasted_iota(jnp.int32, (D, D), 0),
        lax.broadcasted_iota(jnp.int32, (D, D), 1),
    )


def pick(value, lanes):
    return jnp.take_along_axis(value, lanes, axis=1)


def row_of(value, r):
    return jnp.broadcast_to(value[r : r + 1, :], (8, HALF))


def chol_inv(refs):
    nb = len(refs)
    row = lax.broadcasted_iota(jnp.int32, (8, HALF), 0)
    lane = lax.broadcasted_iota(jnp.int32, (8, HALF), 1)
    for h in range(2):
        n0 = h * HALF
        rows = lax.broadcasted_iota(jnp.int32, (D - n0, HALF), 0) + n0
        lanes = lax.broadcasted_iota(jnp.int32, (D - n0, HALF), 1) + n0

        def panel(p, carry, h=h, n0=n0, rows=rows, lanes=lanes):
            j = pl.multiple_of(p * B, B)
            k = pl.multiple_of(n0 + p * B, B)
            first = (lane >= j) & (lane < j + 8)
            second = (lane >= j + 8) & (lane < j + B)
            unit = jnp.where(lane - j == row, 1.0, 0.0)
            unit2 = jnp.where(lane - j - 8 == row, 1.0, 0.0)
            at = [jnp.full((8, HALF), j + c, jnp.int32) for c in range(B)]
            below = rows >= k + B
            own = (lanes >= k) & (lanes < k + B)
            tops = [[a[pl.ds(k, 8), i * HALF : (i + 1) * HALF] for i in range(2)] for a in refs]
            bots = [[a[pl.ds(k + 8, 8), i * HALF : (i + 1) * HALF] for i in range(2)] for a in refs]
            ats = [pick(t[h], at[c]) for c in range(8) for t in tops]
            cts = [ats[n::nb] for n in range(nb)]
            ats = [pick(t[h], at[c]) for c in range(8) for t in bots]
            cbs = [ats[n::nb] for n in range(nb)]
            pts = [jnp.ones((8, HALF), F32) for _ in range(nb)]
            pbs = [jnp.ones((8, HALF), F32) for _ in range(nb)]
            for n in range(nb):
                tops[n][h] = jnp.where(first, unit, tops[n][h])
                bots[n][h] = jnp.where(first, 0.0, bots[n][h])
            for r in range(8):
                for n in range(nb):
                    top, bot, ct, cb = tops[n], bots[n], cts[n], cbs[n]
                    piv = row_of(ct[r], r)
                    inv = 1.0 / piv
                    pts[n] = jnp.where(row == r, piv, pts[n])
                    lt = jnp.where(row > r, ct[r] * inv, 0.0)
                    lb = cb[r] * inv
                    for c in range(r + 1, 8):
                        u = row_of(ct[c], r)
                        ct[c] = ct[c] - lt * u
                        cb[c] = cb[c] - lb * u
                    for i in range(2):
                        u = row_of(top[i], r)
                        if r < 7:
                            top[i] = top[i] - lt * u
                        bot[i] = bot[i] - lb * u
            ats = [pick(t[h], at[8 + c]) for c in range(8) for t in bots]
            cts = [ats[n::nb] for n in range(nb)]
            for n in range(nb):
                tops[n][h] = jnp.where(second, 0.0, tops[n][h])
                bots[n][h] = jnp.where(second, unit2, bots[n][h])
            for r in range(8):
                for n in range(nb):
                    bot, ct = bots[n], cts[n]
                    piv = row_of(ct[r], r)
                    pbs[n] = jnp.where(row == r, piv, pbs[n])
                    if r == 7:
                        continue
                    lb = jnp.where(row > r, ct[r] * (1.0 / piv), 0.0)
                    for c in range(r + 1, 8):
                        ct[c] = ct[c] - lb * row_of(ct[c], r)
                    for i in range(2):
                        bot[i] = bot[i] - lb * row_of(bot[i], r)
            scaled = []
            for n in range(nb):
                rt = lax.rsqrt(pts[n])
                rb = lax.rsqrt(pbs[n])
                scaled.append(
                    jnp.concatenate(
                        [
                            jnp.concatenate([tops[n][0] * rt, tops[n][1] * rt], 1),
                            jnp.concatenate([bots[n][0] * rb, bots[n][1] * rb], 1),
                        ],
                        0,
                    )
                )
            updates = []
            for n in range(nb):
                hi, md, lo = split3(scaled[n])
                left = jnp.concatenate([lo, hi, md, md, hi, hi], 0)
                right = jnp.concatenate([hi, lo, md, hi, md, hi], 0)
                updates.append(dg(left[:, n0:], right, 0, 0))
            for n in range(nb):
                for i in range(2):
                    old = refs[n][n0:, i * HALF : (i + 1) * HALF]
                    kept = jnp.where(own, 0.0, old) if i == h else old
                    now = kept - updates[n][:, i * HALF : (i + 1) * HALF]
                    refs[n][n0:, i * HALF : (i + 1) * HALF] = jnp.where(below, now, old)
                refs[n][pl.ds(k, B), :] = scaled[n]
            return carry

        lax.fori_loop(0, HALF // B, panel, 0)


TABLE = (
    (6, 1, 3, 8, 0, 0, 2, 7, 7, 9),
    (5, 4, 0, 0, 0, 0, 1, 2, 6, 8),
    (4, 5, 3, 6, 0, 0, 2, 5, 9, 8),
    (6, 3, 1, 8, 2, 5, 3, 10, 8, 9),
)


def eye_value():
    r, c = square_iota()
    return jnp.where(r == c, 1.0, 0.0)


def pair_kernel(pos_ref, c_ref, r0, r1, w_ref, v_ref, buf):
    x = pos_ref[1]
    odd = lax.rem(x, 2)
    high = x // 2
    buf[odd] = c_ref[0]
    buf[1 - odd] = r0[...]
    buf[2 + high] = c_ref[1]
    buf[3 - high] = r1[...]
    w_ref[...] = mm(buf[1], buf[0])
    outer = (x == 0) | (x == 3)

    @pl.when(outer)
    def _():
        v_ref[...] = buf[2]

    @pl.when(jnp.logical_not(outer))
    def _():
        v_ref[...] = mm(buf[3], buf[2])


def window_kernel(tab_ref, c_ref, r0, r1, w, q0, q1, prev_ref, t_ref, buf):
    buf[0] = c_ref[0]
    buf[1] = c_ref[1]
    for k, ref in enumerate((r0, r1, w, q0, q1)):
        buf[2 + k] = ref[...]
    buf[7] = eye_value()

    def step(i, _):
        buf[8 + i] = mm(buf[tab_ref[2 * i]], buf[tab_ref[2 * i + 1]])
        return 0

    lax.fori_loop(0, tab_ref[6], step, 0)
    prev_ref[0] = buf[tab_ref[7]]
    prev_ref[1] = buf[tab_ref[8]]
    t_ref[...] = buf[tab_ref[9]]


def entry_kernel(pos_ref, t1, t2, t3, e_ref, buf):
    z = pos_ref[0]
    buf[0] = eye_value()
    for k, ref in enumerate((t1, t2, t3)):
        buf[1 + k] = ref[...]
    e_ref[...] = buf[z]

    def step(i, _):
        e_ref[...] = mm(buf[z - 1 - i], e_ref[...])
        return 0

    lax.fori_loop(0, z - 1, step, 0)


def refinement(y, passes):
    r, c = square_iota()
    err = mm(y, y, 0, 0, passes=3) - jnp.where(r == c, 1.0, 0.0)
    upper = jnp.where(c > r, err, jnp.where(c == r, 0.5 * err, 0.0))
    return mm(y, upper, passes=passes), err


def total_of(value):
    return jnp.sum(jnp.sum(value, axis=0, keepdims=True), axis=1, keepdims=True)


def solve_kernel(
    pos_ref, prev_ref, own, other, c_ref, d_ref, n_ref, r_ref, before_ref, stat_ref, *scratch
):
    refs, m_ref, now = scratch[:4], scratch[4], scratch[5]
    mine = pos_ref[2]
    now[mine] = own[...]
    now[1 - mine] = other[...]

    def products(t, carry):
        left = [jnp.where(t == 0, prev_ref[m], c_ref[m]) for m in range(2)]
        out = [mm(left[m], now[m], passes=SOLVE) for m in range(2)]
        for m in range(2):
            now[m] = out[m]
            m_ref[t, m] = out[m]
        return carry

    lax.fori_loop(0, 2, products, 0)
    for m in range(2):
        before_ref[m] = m_ref[0, m]

    def grams(t, carry):
        out = [mm(m_ref[t, m], m_ref[t, m], 0, 0, passes=GRAM) for m in range(2)]
        for m in range(2):
            now[m] = out[m]

        @pl.when(t == 0)
        def _():
            for m in range(2):
                refs[m][...] = now[m]

        @pl.when(t == 1)
        def _():
            for m in range(2):
                refs[2 + m][...] = now[m]

        return carry

    lax.fori_loop(0, 2, grams, 0)
    chol_inv(refs)
    r, c = square_iota()

    def factors(t, worst):
        inv = [
            jnp.where(c <= r, jnp.where(t == 0, refs[m][...], refs[2 + m][...]), 0.0)
            for m in range(2)
        ]
        ys = [mm(m_ref[t, m], inv[m], 1, 1, passes=SOLVE) for m in range(2)]
        for m in range(2):
            change, err = refinement(ys[m], 1)
            m_ref[t, m] = ys[m] - change
            worst = jnp.maximum(worst, jnp.where(total_of(err * err) < ORTHO2, 0.0, 1.0))
        return worst

    worst = lax.fori_loop(0, 2, factors, jnp.zeros((1, 1), F32))
    stat_ref[...] = jnp.broadcast_to(worst, (8, HALF))

    def results(t, carry):
        left = [jnp.where(t == 0, c_ref[m], d_ref[m]) for m in range(2)]
        part = [mm(left[m], m_ref[t, m], passes=SOLVE) for m in range(2)]
        out = [mm(m_ref[1, m], part[m], 0, 0, passes=SOLVE) for m in range(2)]
        for m in range(2):
            now[m] = out[m]

        @pl.when(t == 0)
        def _():
            for m in range(2):
                r_ref[m] = jnp.where(c >= r, now[m], 0.0)

        @pl.when(t == 1)
        def _():
            for m in range(2):
                n_ref[m] = now[m]

        return carry

    lax.fori_loop(0, 2, results, 0)


def gauge_kernel(pos_ref, prev_ref, c_ref, out_ref, g_ref, b_ref):
    eye = eye_value()
    row = lax.broadcasted_iota(jnp.int32, (8, HALF), 0)
    lane = lax.broadcasted_iota(jnp.int32, (8, HALF), 1)
    norms = []
    for m in range(2):
        full = mm(c_ref[m], prev_ref[m], passes=3)
        gram = mm(full, full, 0, 0, passes=3)
        norm = jnp.sqrt(total_of(gram * gram))
        g_ref[m] = gram / norm
    for m in range(2):
        b_ref[m] = mm(g_ref[m], g_ref[m], passes=3)
    for _ in range(3):
        for m in range(2):
            b_ref[m] = mm(b_ref[m], b_ref[m], passes=3)
    for m in range(2):
        top = jnp.exp(0.0625 * 0.5 * jnp.log(total_of(b_ref[m] * b_ref[m]))) * 1.02
        b_ref[m] = eye - g_ref[m] / top
    for t in range(10):
        for m in range(2):
            b_ref[m] = mm(b_ref[m], b_ref[m], passes=3 if t < 5 else 1)
    out = jnp.zeros((8, HALF), F32)
    for m in range(2):
        norm = jnp.maximum(total_of(b_ref[m] * b_ref[m]), 1.0e-30)
        low = jnp.maximum(1.0 - jnp.exp(jnp.log(norm) / 2048.0), 1.0e-9)
        value = jnp.broadcast_to(-jnp.log(low), (8, HALF))
        out = jnp.where((row == m) & (lane == pos_ref[3]), value, out)
    out_ref[...] = out


def decide_kernel(bound_ref, stat_ref, out_ref):
    v = bound_ref[...]
    lane = lax.broadcasted_iota(jnp.int32, (8, HALF), 1)
    bound = v
    for z in range(3):
        whole = jnp.sum(jnp.where(lane == 4 * z + 3, v, 0.0), axis=1, keepdims=True)
        bound = bound + jnp.where(lane >= 4 * z + 4, whole, 0.0)
    bound = jnp.where(lane < 16, bound, 0.0)
    worst = jnp.max(jnp.max(bound, axis=0, keepdims=True), axis=1, keepdims=True)[0, 0]
    failed = jnp.max(jnp.max(stat_ref[...], axis=0, keepdims=True), axis=1, keepdims=True)[0, 0]
    fine = worst < LIMIT
    out_ref[0] = jnp.where(fine, 0, 16)
    out_ref[1] = jnp.where(fine & (failed > 0.0), 1, 0)


def chain_kernel(before_ref, c_ref, d_ref, n_ref, r_ref, q_ref, a_ref):
    r, c = square_iota()
    lane = lax.broadcasted_iota(jnp.int32, (1, D), 1)

    def orthonormal(m):
        q_ref[m] = n_ref[m]

        def column(k, _):
            a = a_ref[...]
            row = a_ref[pl.ds(k, 1), :]
            pivot = jnp.sum(jnp.where(lane == k, row, 0.0), axis=1, keepdims=True)
            rs = lax.rsqrt(pivot)
            row = jnp.where(lane == k, 1.0, row) * rs
            factor_col = jnp.sum(jnp.where(c == k, a, 0.0), axis=1, keepdims=True) * rs
            below = jnp.where(c == k, 0.0, a) - factor_col * row
            a_ref[...] = jnp.where(r > k, below, jnp.where(r == k, row, a))
            return 0

        def turn(t, carry):
            gram = mm(q_ref[m], q_ref[m], 0, 0)
            mean = total_of(jnp.where(r == c, gram, 0.0)) / D
            shift = jnp.where(t == 0, 1.0e-5, 0.0) * mean
            a_ref[...] = gram + jnp.where(r == c, shift, 0.0)
            lax.fori_loop(0, D, column, 0)
            q_ref[m] = mm(q_ref[m], jnp.where(c <= r, a_ref[...], 0.0), 1, 1)
            return carry

        def again(_, carry):
            q_ref[m] = q_ref[m] - refinement(q_ref[m], 3)[0]
            return carry

        lax.fori_loop(0, 3, turn, 0)
        lax.fori_loop(0, 2, again, 0)

    def one(m, carry):
        def half(t, carry):
            n_ref[m] = jnp.where(t == 0, before_ref[m], mm(c_ref[m], q_ref[m]))
            orthonormal(m)
            return carry

        q_ref[m] = before_ref[m]
        lax.fori_loop(0, 2, half, 0)
        q = q_ref[m]
        r_ref[m] = jnp.where(c >= r, mm(q, n_ref[m], 0, 0), 0.0)
        n_ref[m] = mm(mm(q, d_ref[m], 0, 0), q)
        return carry

    lax.fori_loop(0, 2, one, 0)


def struct(*shape):
    return jax.ShapeDtypeStruct(shape, F32)


VMEM = pl.BlockSpec(memory_space=pltpu.VMEM)
SMEM = pl.BlockSpec(memory_space=pltpu.SMEM)


def call(kernel, outs, scratch, name, table=True):
    def run(*args):
        specs = [VMEM] * len(args)
        if table:
            specs[0] = SMEM
        return pl.pallas_call(
            kernel,
            out_shape=outs,
            in_specs=specs,
            out_specs=jax.tree.map(lambda _: VMEM, outs),
            scratch_shapes=[pltpu.VMEM(shape, F32) for shape in scratch],
            compiler_params=pltpu.CompilerParams(vmem_limit_bytes=48 * 2**20),
            name=name,
        )(*args)

    return run


SQUARE = struct(D, D)
TWO = struct(2, D, D)
TILE = struct(8, HALF)
pair = call(pair_kernel, (SQUARE, SQUARE), [(4, D, D)], "pair")
window = call(window_kernel, (TWO, SQUARE), [(11, D, D)], "window")
entry = call(entry_kernel, SQUARE, [(4, D, D)], "entry")
solve = call(
    solve_kernel,
    (TWO, TWO, TWO, TILE),
    [(D, D)] * 4 + [(2, 2, D, D), (2, D, D)],
    "solve",
)
gauge = call(gauge_kernel, TILE, [(2, D, D), (2, D, D)], "gauge")
chain = call(chain_kernel, (TWO, TWO, TWO), [(D, D)], "chain", table=False)


def decide(bound, stat):
    return pl.pallas_call(
        decide_kernel,
        out_shape=jax.ShapeDtypeStruct((2,), jnp.int32),
        in_specs=[VMEM, VMEM],
        out_specs=SMEM,
        name="decide",
    )(bound, stat)


def x_move(value, to):
    return lax.ppermute(value, "row", [(i, (i // 4) * 4 + to(i % 4)) for i in range(16)])


def z_move(value, s):
    return lax.ppermute(value, "row", [(i, i + 4 * s) for i in range(16 - 4 * s)])


def z_ring(value, s):
    return lax.ppermute(value, "row", [(i, (i + 4 * s) % 16) for i in range(16)])


def x_pairs(value):
    return x_move(value, lambda x: x ^ 1)


def x_mirror(value):
    return x_move(value, lambda x: 3 - x)


def largest_in_row(value):
    moved = [x_move(value, lambda x, s=s: (x + s) % 4) for s in (1, 2, 3)]
    value = functools.reduce(jnp.maximum, moved, value)
    return functools.reduce(jnp.maximum, [z_ring(value, s) for s in (1, 2, 3)], value)


def shards(diag_blocks, coupling_blocks):
    diagonal = diag_blocks.reshape(2, D, D)
    coupling = coupling_blocks.reshape(2, D, D)
    position = lax.axis_index("row")
    z, x = position // 4, position % 4
    mine = jnp.where((x == 0) | (x == 3), 1, 0)
    pos = jnp.stack([z, x, mine, position]).astype(jnp.int32)
    table = jnp.asarray(TABLE, jnp.int32)[x]

    r0, r1 = x_pairs(coupling[0]), x_mirror(coupling[1])
    w, v = pair(pos, coupling, r0, r1)
    q0, q1 = x_mirror(w), x_pairs(v)
    prev, total = window(table, coupling, r0, r1, w, q0, q1)
    below = [z_move(total, s) for s in (1, 2, 3)]
    bound = largest_in_row(gauge(pos, prev, coupling))
    own = entry(pos, *below)
    new, tri, before, stat = solve(pos, prev, own, x_pairs(own), coupling, diagonal)
    rounds = decide(bound, stat)

    def local(_, carried):
        new, tri, q = chain(carried[0], coupling, diagonal)
        return q, new, tri

    _, new, tri = lax.fori_loop(0, rounds[1], local, (before, new, tri))

    def step(i, carried):
        q, new, tri = carried
        new_now, tri_now, q = chain(q, coupling, diagonal)
        keep = i == position
        new = jnp.where(keep, new_now, new)
        tri = jnp.where(keep, tri_now, tri)
        return lax.ppermute(q, "row", [(j, j + 1) for j in range(15)]), new, tri

    eyes = jnp.broadcast_to(jnp.eye(D, dtype=F32), (2, D, D))
    _, new, tri = lax.fori_loop(0, rounds[0], step, (eyes, new, tri))
    shape = diag_blocks.shape
    return new.reshape(shape), tri.reshape(shape)


def solution(mesh):
    placed = P("section", None, "row", None, None)
    return jax.shard_map(
        shards,
        mesh=mesh,
        in_specs=(placed, placed),
        out_specs=(placed, placed),
        check_vma=False,
    )
```

```python
import functools

import jax
import jax.numpy as jnp
from jax import lax
from jax.experimental import pallas as pl
from jax.experimental.pallas import tpu as pltpu
from jax.sharding import PartitionSpec as P

D = 256
B = 16
HALF = 128
SOLVE = 3
GRAM = 6
F32 = jnp.float32
BF16 = jnp.bfloat16
LIMIT = 17.97
ORTHO2 = 4.0e-4


def dg(a, b, ca, cb):
    return lax.dot_general(a, b, (((ca,), (cb,)), ((), ())), preferred_element_type=F32)


def split2(x):
    h = x.astype(BF16)
    return h, (x - h.astype(F32)).astype(BF16)


def split3(x):
    h = x.astype(BF16)
    r = x - h.astype(F32)
    m = r.astype(BF16)
    return h, m, (r - m.astype(F32)).astype(BF16)


def mm(a, b, ca=1, cb=0, passes=6):
    if passes == 1:
        return dg(a.astype(BF16), b.astype(BF16), ca, cb)
    if passes == 3:
        ah, al = split2(a)
        bh, bl = split2(b)
        return dg(al, bh, ca, cb) + dg(ah, bl, ca, cb) + dg(ah, bh, ca, cb)
    ah, am, al = split3(a)
    bh, bm, bl = split3(b)
    small = dg(al, bh, ca, cb) + dg(ah, bl, ca, cb) + dg(am, bm, ca, cb)
    return (small + (dg(am, bh, ca, cb) + dg(ah, bm, ca, cb))) + dg(ah, bh, ca, cb)


def square_iota():
    return (
        lax.broadcasted_iota(jnp.int32, (D, D), 0),
        lax.broadcasted_iota(jnp.int32, (D, D), 1),
    )


def pick(value, lanes):
    return jnp.take_along_axis(value, lanes, axis=1)


def row_of(value, r):
    return jnp.broadcast_to(value[r : r + 1, :], (8, HALF))


def chol_inv(refs):
    nb = len(refs)
    row = lax.broadcasted_iota(jnp.int32, (8, HALF), 0)
    lane = lax.broadcasted_iota(jnp.int32, (8, HALF), 1)
    for h in range(2):
        n0 = h * HALF
        rows = lax.broadcasted_iota(jnp.int32, (D - n0, HALF), 0) + n0
        lanes = lax.broadcasted_iota(jnp.int32, (D - n0, HALF), 1) + n0

        def panel(p, carry, h=h, n0=n0, rows=rows, lanes=lanes):
            j = pl.multiple_of(p * B, B)
            k = pl.multiple_of(n0 + p * B, B)
            first = (lane >= j) & (lane < j + 8)
            second = (lane >= j + 8) & (lane < j + B)
            unit = jnp.where(lane - j == row, 1.0, 0.0)
            unit2 = jnp.where(lane - j - 8 == row, 1.0, 0.0)
            at = [jnp.full((8, HALF), j + c, jnp.int32) for c in range(B)]
            below = rows >= k + B
            own = (lanes >= k) & (lanes < k + B)
            tops = [[a[pl.ds(k, 8), i * HALF : (i + 1) * HALF] for i in range(2)] for a in refs]
            bots = [[a[pl.ds(k + 8, 8), i * HALF : (i + 1) * HALF] for i in range(2)] for a in refs]
            ats = [pick(t[h], at[c]) for c in range(8) for t in tops]
            cts = [ats[n::nb] for n in range(nb)]
            ats = [pick(t[h], at[c]) for c in range(8) for t in bots]
            cbs = [ats[n::nb] for n in range(nb)]
            pts = [jnp.ones((8, HALF), F32) for _ in range(nb)]
            pbs = [jnp.ones((8, HALF), F32) for _ in range(nb)]
            for n in range(nb):
                tops[n][h] = jnp.where(first, unit, tops[n][h])
                bots[n][h] = jnp.where(first, 0.0, bots[n][h])
            for r in range(8):
                for n in range(nb):
                    top, bot, ct, cb = tops[n], bots[n], cts[n], cbs[n]
                    piv = row_of(ct[r], r)
                    inv = 1.0 / piv
                    pts[n] = jnp.where(row == r, piv, pts[n])
                    lt = jnp.where(row > r, ct[r] * inv, 0.0)
                    lb = cb[r] * inv
                    for c in range(r + 1, 8):
                        u = row_of(ct[c], r)
                        ct[c] = ct[c] - lt * u
                        cb[c] = cb[c] - lb * u
                    for i in range(2):
                        u = row_of(top[i], r)
                        if r < 7:
                            top[i] = top[i] - lt * u
                        bot[i] = bot[i] - lb * u
            ats = [pick(t[h], at[8 + c]) for c in range(8) for t in bots]
            cts = [ats[n::nb] for n in range(nb)]
            for n in range(nb):
                tops[n][h] = jnp.where(second, 0.0, tops[n][h])
                bots[n][h] = jnp.where(second, unit2, bots[n][h])
            for r in range(8):
                for n in range(nb):
                    bot, ct = bots[n], cts[n]
                    piv = row_of(ct[r], r)
                    pbs[n] = jnp.where(row == r, piv, pbs[n])
                    if r == 7:
                        continue
                    lb = jnp.where(row > r, ct[r] * (1.0 / piv), 0.0)
                    for c in range(r + 1, 8):
                        ct[c] = ct[c] - lb * row_of(ct[c], r)
                    for i in range(2):
                        bot[i] = bot[i] - lb * row_of(bot[i], r)
            scaled = []
            for n in range(nb):
                rt = lax.rsqrt(pts[n])
                rb = lax.rsqrt(pbs[n])
                scaled.append(
                    jnp.concatenate(
                        [
                            jnp.concatenate([tops[n][0] * rt, tops[n][1] * rt], 1),
                            jnp.concatenate([bots[n][0] * rb, bots[n][1] * rb], 1),
                        ],
                        0,
                    )
                )
            updates = []
            for n in range(nb):
                hi, md, lo = split3(scaled[n])
                left = jnp.concatenate([lo, hi, md, md, hi, hi], 0)
                right = jnp.concatenate([hi, lo, md, hi, md, hi], 0)
                updates.append(dg(left[:, n0:], right, 0, 0))
            for n in range(nb):
                for i in range(2):
                    old = refs[n][n0:, i * HALF : (i + 1) * HALF]
                    kept = jnp.where(own, 0.0, old) if i == h else old
                    now = kept - updates[n][:, i * HALF : (i + 1) * HALF]
                    refs[n][n0:, i * HALF : (i + 1) * HALF] = jnp.where(below, now, old)
                refs[n][pl.ds(k, B), :] = scaled[n]
            return carry

        lax.fori_loop(0, HALF // B, panel, 0)


TABLE = (
    (6, 1, 3, 8, 0, 0, 2, 7, 7, 9),
    (5, 4, 0, 0, 0, 0, 1, 2, 6, 8),
    (4, 5, 3, 6, 0, 0, 2, 5, 9, 8),
    (6, 3, 1, 8, 2, 5, 3, 10, 8, 9),
)


def eye_value():
    r, c = square_iota()
    return jnp.where(r == c, 1.0, 0.0)


def pair_kernel(pos_ref, c_ref, r0, r1, w_ref, v_ref, buf):
    x = pos_ref[1]
    odd = lax.rem(x, 2)
    high = x // 2
    buf[odd] = c_ref[0]
    buf[1 - odd] = r0[...]
    buf[2 + high] = c_ref[1]
    buf[3 - high] = r1[...]
    w_ref[...] = mm(buf[1], buf[0])
    outer = (x == 0) | (x == 3)

    @pl.when(outer)
    def _():
        v_ref[...] = buf[2]

    @pl.when(jnp.logical_not(outer))
    def _():
        v_ref[...] = mm(buf[3], buf[2])


def window_kernel(tab_ref, c_ref, r0, r1, w, q0, q1, prev_ref, t_ref, buf):
    buf[0] = c_ref[0]
    buf[1] = c_ref[1]
    for k, ref in enumerate((r0, r1, w, q0, q1)):
        buf[2 + k] = ref[...]
    buf[7] = eye_value()

    def step(i, _):
        buf[8 + i] = mm(buf[tab_ref[2 * i]], buf[tab_ref[2 * i + 1]])
        return 0

    lax.fori_loop(0, tab_ref[6], step, 0)
    prev_ref[0] = buf[tab_ref[7]]
    prev_ref[1] = buf[tab_ref[8]]
    t_ref[...] = buf[tab_ref[9]]


def entry_kernel(pos_ref, t1, t2, t3, e_ref, buf):
    z = pos_ref[0]
    buf[0] = eye_value()
    for k, ref in enumerate((t1, t2, t3)):
        buf[1 + k] = ref[...]
    e_ref[...] = buf[z]

    def step(i, _):
        e_ref[...] = mm(buf[z - 1 - i], e_ref[...])
        return 0

    lax.fori_loop(0, z - 1, step, 0)


def refinement(y, passes):
    r, c = square_iota()
    err = mm(y, y, 0, 0, passes=3) - jnp.where(r == c, 1.0, 0.0)
    upper = jnp.where(c > r, err, jnp.where(c == r, 0.5 * err, 0.0))
    return mm(y, upper, passes=passes), err


def total_of(value):
    return jnp.sum(jnp.sum(value, axis=0, keepdims=True), axis=1, keepdims=True)


def solve_kernel(
    pos_ref,
    prev_ref,
    own,
    other,
    c_ref,
    d_ref,
    bound_ref,
    n_ref,
    r_ref,
    before_ref,
    trips_ref,
    whole_ref,
    *scratch,
):
    refs, m_ref, now = scratch[:4], scratch[4], scratch[5]
    mine = pos_ref[2]
    now[mine] = own[...]
    now[1 - mine] = other[...]

    def products(t, carry):
        left = [jnp.where(t == 0, prev_ref[m], c_ref[m]) for m in range(2)]
        out = [mm(left[m], now[m], passes=SOLVE) for m in range(2)]
        for m in range(2):
            now[m] = out[m]
            m_ref[t, m] = out[m]
        return carry

    lax.fori_loop(0, 2, products, 0)
    for m in range(2):
        before_ref[m] = m_ref[0, m]

    def grams(t, carry):
        out = [mm(m_ref[t, m], m_ref[t, m], 0, 0, passes=GRAM) for m in range(2)]
        for m in range(2):
            now[m] = out[m]

        @pl.when(t == 0)
        def _():
            for m in range(2):
                refs[m][...] = now[m]

        @pl.when(t == 1)
        def _():
            for m in range(2):
                refs[2 + m][...] = now[m]

        return carry

    lax.fori_loop(0, 2, grams, 0)
    chol_inv(refs)
    r, c = square_iota()

    def factors(t, worst):
        inv = [
            jnp.where(c <= r, jnp.where(t == 0, refs[m][...], refs[2 + m][...]), 0.0)
            for m in range(2)
        ]
        ys = [mm(m_ref[t, m], inv[m], 1, 1, passes=SOLVE) for m in range(2)]
        for m in range(2):
            change, err = refinement(ys[m], 1)
            m_ref[t, m] = ys[m] - change
            worst = jnp.maximum(worst, jnp.where(total_of(err * err) < ORTHO2, 0.0, 1.0))
        return worst

    worst = lax.fori_loop(0, 2, factors, jnp.zeros((1, 1), F32))
    fine = bound_of(bound_ref[...]) < LIMIT
    trips_ref[0] = jnp.where(fine, jnp.where(worst[0, 0] > 0.0, 1, 0), 16)
    whole_ref[0] = jnp.where(fine, 0, 1)

    def results(t, carry):
        left = [jnp.where(t == 0, c_ref[m], d_ref[m]) for m in range(2)]
        part = [mm(left[m], m_ref[t, m], passes=SOLVE) for m in range(2)]
        out = [mm(m_ref[1, m], part[m], 0, 0, passes=SOLVE) for m in range(2)]
        for m in range(2):
            now[m] = out[m]

        @pl.when(t == 0)
        def _():
            for m in range(2):
                r_ref[m] = jnp.where(c >= r, now[m], 0.0)

        @pl.when(t == 1)
        def _():
            for m in range(2):
                n_ref[m] = now[m]

        return carry

    lax.fori_loop(0, 2, results, 0)


def gauge_kernel(pos_ref, prev_ref, c_ref, out_ref, g_ref, b_ref):
    eye = eye_value()
    row = lax.broadcasted_iota(jnp.int32, (8, HALF), 0)
    lane = lax.broadcasted_iota(jnp.int32, (8, HALF), 1)
    norms = []
    for m in range(2):
        full = mm(c_ref[m], prev_ref[m], passes=3)
        gram = mm(full, full, 0, 0, passes=3)
        norm = jnp.sqrt(total_of(gram * gram))
        g_ref[m] = gram / norm
    for m in range(2):
        b_ref[m] = mm(g_ref[m], g_ref[m], passes=3)
    for _ in range(3):
        for m in range(2):
            b_ref[m] = mm(b_ref[m], b_ref[m], passes=3)
    for m in range(2):
        top = jnp.exp(0.0625 * 0.5 * jnp.log(total_of(b_ref[m] * b_ref[m]))) * 1.02
        b_ref[m] = eye - g_ref[m] / top
    for t in range(10):
        for m in range(2):
            b_ref[m] = mm(b_ref[m], b_ref[m], passes=3 if t < 5 else 1)
    out = jnp.zeros((8, HALF), F32)
    for m in range(2):
        norm = jnp.maximum(total_of(b_ref[m] * b_ref[m]), 1.0e-30)
        low = jnp.maximum(1.0 - jnp.exp(jnp.log(norm) / 2048.0), 1.0e-9)
        value = jnp.broadcast_to(-jnp.log(low), (8, HALF))
        out = jnp.where((row == m) & (lane == pos_ref[3]), value, out)
    out_ref[...] = out


def bound_of(v):
    lane = lax.broadcasted_iota(jnp.int32, (8, HALF), 1)
    bound = v
    for z in range(3):
        whole = jnp.sum(jnp.where(lane == 4 * z + 3, v, 0.0), axis=1, keepdims=True)
        bound = bound + jnp.where(lane >= 4 * z + 4, whole, 0.0)
    bound = jnp.where(lane < 16, bound, 0.0)
    return jnp.max(jnp.max(bound, axis=0, keepdims=True), axis=1, keepdims=True)[0, 0]


def struct(*shape):
    return jax.ShapeDtypeStruct(shape, F32)


VMEM = pl.BlockSpec(memory_space=pltpu.VMEM)
SMEM = pl.BlockSpec(memory_space=pltpu.SMEM)


def call(kernel, outs, scratch, name, table=True):
    def run(*args):
        specs = [VMEM] * len(args)
        if table:
            specs[0] = SMEM
        return pl.pallas_call(
            kernel,
            out_shape=outs,
            in_specs=specs,
            out_specs=jax.tree.map(lambda o: SMEM if o.dtype == jnp.int32 else VMEM, outs),
            scratch_shapes=[pltpu.VMEM(shape, F32) for shape in scratch],
            compiler_params=pltpu.CompilerParams(vmem_limit_bytes=48 * 2**20),
            name=name,
        )(*args)

    return run


SQUARE = struct(D, D)
TWO = struct(2, D, D)
TILE = struct(8, HALF)
COUNT = jax.ShapeDtypeStruct((1,), jnp.int32)
pair = call(pair_kernel, (SQUARE, SQUARE), [(4, D, D)], "pair")
window = call(window_kernel, (TWO, SQUARE), [(11, D, D)], "window")
entry = call(entry_kernel, SQUARE, [(4, D, D)], "entry")
solve = call(
    solve_kernel,
    (TWO, TWO, TWO, COUNT, COUNT),
    [(D, D)] * 4 + [(2, 2, D, D), (2, D, D)],
    "solve",
)
gauge = call(gauge_kernel, TILE, [(2, D, D), (2, D, D)], "gauge")


highest = lax.Precision.HIGHEST


def product(left, right):
    return jnp.matmul(left, right, precision=highest, preferred_element_type=F32)


def flip(value):
    return jnp.swapaxes(value, -1, -2)


def orthonormal(panel):
    def turn(t, y):
        gram = product(flip(y), y)
        mean = jnp.trace(gram, axis1=-2, axis2=-1)[:, None, None] / D
        gram = gram + jnp.where(t == 0, 1.0e-5, 0.0) * mean * jnp.eye(D, dtype=F32)
        lower = jnp.linalg.cholesky(gram)
        return flip(lax.linalg.triangular_solve(lower, flip(y), left_side=True, lower=True))

    return lax.fori_loop(0, 3, turn, panel)


def one_block(before, coupling, diagonal):
    def half(t, carried):
        panel, q = carried
        panel = jnp.where(t == 0, panel, product(coupling, q))
        return panel, orthonormal(panel)

    panel, q = lax.fori_loop(0, 2, half, (before, before))
    new = product(product(flip(q), diagonal), q)
    return new, jnp.triu(product(flip(q), panel)), q


def x_move(value, to):
    return lax.ppermute(value, "row", [(i, (i // 4) * 4 + to(i % 4)) for i in range(16)])


def z_move(value, s):
    return lax.ppermute(value, "row", [(i, i + 4 * s) for i in range(16 - 4 * s)])


def z_ring(value, s):
    return lax.ppermute(value, "row", [(i, (i + 4 * s) % 16) for i in range(16)])


def x_pairs(value):
    return x_move(value, lambda x: x ^ 1)


def x_mirror(value):
    return x_move(value, lambda x: 3 - x)


def largest_in_row(value):
    moved = [x_move(value, lambda x, s=s: (x + s) % 4) for s in (1, 2, 3)]
    value = functools.reduce(jnp.maximum, moved, value)
    return functools.reduce(jnp.maximum, [z_ring(value, s) for s in (1, 2, 3)], value)


def shards(diag_blocks, coupling_blocks):
    diagonal = diag_blocks.reshape(2, D, D)
    coupling = coupling_blocks.reshape(2, D, D)
    position = lax.axis_index("row")
    z, x = position // 4, position % 4
    mine = jnp.where((x == 0) | (x == 3), 1, 0)
    pos = jnp.stack([z, x, mine, position]).astype(jnp.int32)
    table = jnp.asarray(TABLE, jnp.int32)[x]

    r0, r1 = x_pairs(coupling[0]), x_mirror(coupling[1])
    w, v = pair(pos, coupling, r0, r1)
    q0, q1 = x_mirror(w), x_pairs(v)
    prev, total = window(table, coupling, r0, r1, w, q0, q1)
    below = [z_move(total, s) for s in (1, 2, 3)]
    gauged = gauge(pos, prev, coupling)
    own = entry(pos, *below)
    gauged, own = lax.optimization_barrier((gauged, own))
    other = x_pairs(own)
    bound = largest_in_row(gauged)
    new, tri, before, trips, whole = solve(
        pos, prev, own, other, coupling, diagonal, bound
    )
    whole = whole.reshape(()) > 0

    def step(i, carried):
        q, new, tri = carried
        q = jnp.where(whole & (i == 0), jnp.eye(D, dtype=F32), q)
        new_now, tri_now, q = one_block(q, coupling, diagonal)
        keep = (i == position) | jnp.logical_not(whole)
        new = jnp.where(keep, new_now, new)
        tri = jnp.where(keep, tri_now, tri)
        q = lax.cond(
            whole,
            lambda q: lax.ppermute(q, "row", [(j, j + 1) for j in range(15)]),
            lambda q: q,
            q,
        )
        return q, new, tri

    _, new, tri = lax.fori_loop(0, trips.reshape(()), step, (before, new, tri))
    shape = diag_blocks.shape
    return new.reshape(shape), tri.reshape(shape)


def solution(mesh):
    placed = P("section", None, "row", None, None)
    return jax.shard_map(
        shards,
        mesh=mesh,
        in_specs=(placed, placed),
        out_specs=(placed, placed),
        check_vma=False,
    )
```

```python
import functools

import jax
import jax.numpy as jnp
from jax import lax
from jax.experimental import pallas as pl
from jax.experimental.pallas import tpu as pltpu
from jax.sharding import PartitionSpec as P

D = 256
B = 16
HALF = 128
SOLVE = 3
GRAM = 6
F32 = jnp.float32
BF16 = jnp.bfloat16
LIMIT = 17.97
ORTHO2 = 4.0e-4


def dg(a, b, ca, cb):
    return lax.dot_general(a, b, (((ca,), (cb,)), ((), ())), preferred_element_type=F32)


def split2(x):
    h = x.astype(BF16)
    return h, (x - h.astype(F32)).astype(BF16)


def split3(x):
    h = x.astype(BF16)
    r = x - h.astype(F32)
    m = r.astype(BF16)
    return h, m, (r - m.astype(F32)).astype(BF16)


def mm(a, b, ca=1, cb=0, passes=6):
    if passes == 1:
        return dg(a.astype(BF16), b.astype(BF16), ca, cb)
    if passes == 3:
        ah, al = split2(a)
        bh, bl = split2(b)
        return dg(al, bh, ca, cb) + dg(ah, bl, ca, cb) + dg(ah, bh, ca, cb)
    ah, am, al = split3(a)
    bh, bm, bl = split3(b)
    small = dg(al, bh, ca, cb) + dg(ah, bl, ca, cb) + dg(am, bm, ca, cb)
    return (small + (dg(am, bh, ca, cb) + dg(ah, bm, ca, cb))) + dg(ah, bh, ca, cb)


def square_iota():
    return (
        lax.broadcasted_iota(jnp.int32, (D, D), 0),
        lax.broadcasted_iota(jnp.int32, (D, D), 1),
    )


def pick(value, lanes):
    return jnp.take_along_axis(value, lanes, axis=1)


def row_of(value, r):
    return jnp.broadcast_to(value[r : r + 1, :], (8, HALF))


def chol_inv(refs):
    nb = len(refs)
    row = lax.broadcasted_iota(jnp.int32, (8, HALF), 0)
    lane = lax.broadcasted_iota(jnp.int32, (8, HALF), 1)
    for h in range(2):
        n0 = h * HALF
        rows = lax.broadcasted_iota(jnp.int32, (D - n0, HALF), 0) + n0
        lanes = lax.broadcasted_iota(jnp.int32, (D - n0, HALF), 1) + n0

        def panel(p, carry, h=h, n0=n0, rows=rows, lanes=lanes):
            j = pl.multiple_of(p * B, B)
            k = pl.multiple_of(n0 + p * B, B)
            first = (lane >= j) & (lane < j + 8)
            second = (lane >= j + 8) & (lane < j + B)
            unit = jnp.where(lane - j == row, 1.0, 0.0)
            unit2 = jnp.where(lane - j - 8 == row, 1.0, 0.0)
            at = [jnp.full((8, HALF), j + c, jnp.int32) for c in range(B)]
            below = rows >= k + B
            own = (lanes >= k) & (lanes < k + B)
            tops = [[a[pl.ds(k, 8), i * HALF : (i + 1) * HALF] for i in range(2)] for a in refs]
            bots = [[a[pl.ds(k + 8, 8), i * HALF : (i + 1) * HALF] for i in range(2)] for a in refs]
            ats = [pick(t[h], at[c]) for c in range(8) for t in tops]
            cts = [ats[n::nb] for n in range(nb)]
            ats = [pick(t[h], at[c]) for c in range(8) for t in bots]
            cbs = [ats[n::nb] for n in range(nb)]
            pts = [jnp.ones((8, HALF), F32) for _ in range(nb)]
            pbs = [jnp.ones((8, HALF), F32) for _ in range(nb)]
            for n in range(nb):
                tops[n][h] = jnp.where(first, unit, tops[n][h])
                bots[n][h] = jnp.where(first, 0.0, bots[n][h])
            for r in range(8):
                for n in range(nb):
                    top, bot, ct, cb = tops[n], bots[n], cts[n], cbs[n]
                    piv = row_of(ct[r], r)
                    inv = 1.0 / piv
                    pts[n] = jnp.where(row == r, piv, pts[n])
                    lt = jnp.where(row > r, ct[r] * inv, 0.0)
                    lb = cb[r] * inv
                    for c in range(r + 1, 8):
                        u = row_of(ct[c], r)
                        ct[c] = ct[c] - lt * u
                        cb[c] = cb[c] - lb * u
                    for i in range(2):
                        u = row_of(top[i], r)
                        if r < 7:
                            top[i] = top[i] - lt * u
                        bot[i] = bot[i] - lb * u
            ats = [pick(t[h], at[8 + c]) for c in range(8) for t in bots]
            cts = [ats[n::nb] for n in range(nb)]
            for n in range(nb):
                tops[n][h] = jnp.where(second, 0.0, tops[n][h])
                bots[n][h] = jnp.where(second, unit2, bots[n][h])
            for r in range(8):
                for n in range(nb):
                    bot, ct = bots[n], cts[n]
                    piv = row_of(ct[r], r)
                    pbs[n] = jnp.where(row == r, piv, pbs[n])
                    if r == 7:
                        continue
                    lb = jnp.where(row > r, ct[r] * (1.0 / piv), 0.0)
                    for c in range(r + 1, 8):
                        ct[c] = ct[c] - lb * row_of(ct[c], r)
                    for i in range(2):
                        bot[i] = bot[i] - lb * row_of(bot[i], r)
            scaled = []
            for n in range(nb):
                rt = lax.rsqrt(pts[n])
                rb = lax.rsqrt(pbs[n])
                scaled.append(
                    jnp.concatenate(
                        [
                            jnp.concatenate([tops[n][0] * rt, tops[n][1] * rt], 1),
                            jnp.concatenate([bots[n][0] * rb, bots[n][1] * rb], 1),
                        ],
                        0,
                    )
                )
            updates = []
            for n in range(nb):
                hi, md, lo = split3(scaled[n])
                left = jnp.concatenate([lo, hi, md, md, hi, hi], 0)
                right = jnp.concatenate([hi, lo, md, hi, md, hi], 0)
                updates.append(dg(left[:, n0:], right, 0, 0))
            for n in range(nb):
                for i in range(2):
                    old = refs[n][n0:, i * HALF : (i + 1) * HALF]
                    kept = jnp.where(own, 0.0, old) if i == h else old
                    now = kept - updates[n][:, i * HALF : (i + 1) * HALF]
                    refs[n][n0:, i * HALF : (i + 1) * HALF] = jnp.where(below, now, old)
                refs[n][pl.ds(k, B), :] = scaled[n]
            return carry

        lax.fori_loop(0, HALF // B, panel, 0)


TABLE = (
    (6, 1, 3, 8, 0, 0, 2, 7, 7, 9),
    (5, 4, 0, 0, 0, 0, 1, 2, 6, 8),
    (4, 5, 3, 6, 0, 0, 2, 5, 9, 8),
    (6, 3, 1, 8, 2, 5, 3, 10, 8, 9),
)


def eye_value():
    r, c = square_iota()
    return jnp.where(r == c, 1.0, 0.0)


def pair_kernel(pos_ref, c_ref, r0, r1, w_ref, v_ref, buf):
    x = pos_ref[1]
    odd = lax.rem(x, 2)
    high = x // 2
    buf[odd] = c_ref[0]
    buf[1 - odd] = r0[...]
    buf[2 + high] = c_ref[1]
    buf[3 - high] = r1[...]
    w_ref[...] = mm(buf[1], buf[0])
    outer = (x == 0) | (x == 3)

    @pl.when(outer)
    def _():
        v_ref[...] = buf[2]

    @pl.when(jnp.logical_not(outer))
    def _():
        v_ref[...] = mm(buf[3], buf[2])


def window_kernel(tab_ref, c_ref, r0, r1, w, q0, q1, prev_ref, t_ref, buf):
    buf[0] = c_ref[0]
    buf[1] = c_ref[1]
    for k, ref in enumerate((r0, r1, w, q0, q1)):
        buf[2 + k] = ref[...]
    buf[7] = eye_value()

    def step(i, _):
        buf[8 + i] = mm(buf[tab_ref[2 * i]], buf[tab_ref[2 * i + 1]])
        return 0

    lax.fori_loop(0, tab_ref[6], step, 0)
    prev_ref[0] = buf[tab_ref[7]]
    prev_ref[1] = buf[tab_ref[8]]
    t_ref[...] = buf[tab_ref[9]]


def entry_kernel(pos_ref, t1, t2, t3, e_ref, buf):
    z = pos_ref[0]
    buf[0] = eye_value()
    for k, ref in enumerate((t1, t2, t3)):
        buf[1 + k] = ref[...]
    e_ref[...] = buf[z]

    def step(i, _):
        e_ref[...] = mm(buf[z - 1 - i], e_ref[...])
        return 0

    lax.fori_loop(0, z - 1, step, 0)


def refinement(y, passes):
    r, c = square_iota()
    err = mm(y, y, 0, 0, passes=3) - jnp.where(r == c, 1.0, 0.0)
    upper = jnp.where(c > r, err, jnp.where(c == r, 0.5 * err, 0.0))
    return mm(y, upper, passes=passes), err


def total_of(value):
    return jnp.sum(jnp.sum(value, axis=0, keepdims=True), axis=1, keepdims=True)


def solve_kernel(
    pos_ref,
    prev_ref,
    own,
    other,
    c_ref,
    d_ref,
    bound_ref,
    n_ref,
    r_ref,
    before_ref,
    trips_ref,
    whole_ref,
    *scratch,
):
    refs, m_ref, now = scratch[:4], scratch[4], scratch[5]
    mine = pos_ref[2]
    now[mine] = own[...]
    now[1 - mine] = other[...]

    def products(t, carry):
        left = [jnp.where(t == 0, prev_ref[m], c_ref[m]) for m in range(2)]
        out = [mm(left[m], now[m], passes=SOLVE) for m in range(2)]
        for m in range(2):
            now[m] = out[m]
            m_ref[t, m] = out[m]
        return carry

    lax.fori_loop(0, 2, products, 0)
    for m in range(2):
        before_ref[m] = m_ref[0, m]

    def grams(t, carry):
        out = [mm(m_ref[t, m], m_ref[t, m], 0, 0, passes=GRAM) for m in range(2)]
        for m in range(2):
            now[m] = out[m]

        @pl.when(t == 0)
        def _():
            for m in range(2):
                refs[m][...] = now[m]

        @pl.when(t == 1)
        def _():
            for m in range(2):
                refs[2 + m][...] = now[m]

        return carry

    lax.fori_loop(0, 2, grams, 0)
    chol_inv(refs)
    r, c = square_iota()

    def factors(t, worst):
        inv = [
            jnp.where(c <= r, jnp.where(t == 0, refs[m][...], refs[2 + m][...]), 0.0)
            for m in range(2)
        ]
        ys = [mm(m_ref[t, m], inv[m], 1, 1, passes=SOLVE) for m in range(2)]
        for m in range(2):
            change, err = refinement(ys[m], 1)
            m_ref[t, m] = ys[m] - change
            worst = jnp.maximum(worst, jnp.where(total_of(err * err) < ORTHO2, 0.0, 1.0))
        return worst

    worst = lax.fori_loop(0, 2, factors, jnp.zeros((1, 1), F32))
    fine = bound_of(bound_ref[...]) < LIMIT
    trips_ref[0] = jnp.where(fine, jnp.where(worst[0, 0] > 0.0, 1, 0), 16)
    whole_ref[0] = jnp.where(fine, 0, 1)

    def results(t, carry):
        left = [jnp.where(t == 0, c_ref[m], d_ref[m]) for m in range(2)]
        part = [mm(left[m], m_ref[t, m], passes=SOLVE) for m in range(2)]
        out = [mm(m_ref[1, m], part[m], 0, 0, passes=SOLVE) for m in range(2)]
        for m in range(2):
            now[m] = out[m]

        @pl.when(t == 0)
        def _():
            for m in range(2):
                r_ref[m] = jnp.where(c >= r, now[m], 0.0)

        @pl.when(t == 1)
        def _():
            for m in range(2):
                n_ref[m] = now[m]

        return carry

    lax.fori_loop(0, 2, results, 0)


def gauge_kernel(pos_ref, prev_ref, c_ref, out_ref, g_ref, b_ref):
    eye = eye_value()
    row = lax.broadcasted_iota(jnp.int32, (8, HALF), 0)
    lane = lax.broadcasted_iota(jnp.int32, (8, HALF), 1)
    norms = []
    for m in range(2):
        full = mm(c_ref[m], prev_ref[m], passes=3)
        gram = mm(full, full, 0, 0, passes=3)
        norm = jnp.sqrt(total_of(gram * gram))
        g_ref[m] = gram / norm
    for m in range(2):
        b_ref[m] = mm(g_ref[m], g_ref[m], passes=3)
    for _ in range(3):
        for m in range(2):
            b_ref[m] = mm(b_ref[m], b_ref[m], passes=3)
    for m in range(2):
        top = jnp.exp(0.0625 * 0.5 * jnp.log(total_of(b_ref[m] * b_ref[m]))) * 1.02
        b_ref[m] = eye - g_ref[m] / top
    for t in range(10):
        for m in range(2):
            b_ref[m] = mm(b_ref[m], b_ref[m], passes=3 if t < 5 else 1)
    out = jnp.zeros((8, HALF), F32)
    for m in range(2):
        norm = jnp.maximum(total_of(b_ref[m] * b_ref[m]), 1.0e-30)
        low = jnp.maximum(1.0 - jnp.exp(jnp.log(norm) / 2048.0), 1.0e-9)
        value = jnp.broadcast_to(-jnp.log(low), (8, HALF))
        out = jnp.where((row == m) & (lane == pos_ref[3]), value, out)
    out_ref[...] = out


def bound_of(v):
    lane = lax.broadcasted_iota(jnp.int32, (8, HALF), 1)
    bound = v
    for z in range(3):
        whole = jnp.sum(jnp.where(lane == 4 * z + 3, v, 0.0), axis=1, keepdims=True)
        bound = bound + jnp.where(lane >= 4 * z + 4, whole, 0.0)
    bound = jnp.where(lane < 16, bound, 0.0)
    return jnp.max(jnp.max(bound, axis=0, keepdims=True), axis=1, keepdims=True)[0, 0]


def struct(*shape):
    return jax.ShapeDtypeStruct(shape, F32)


VMEM = pl.BlockSpec(memory_space=pltpu.VMEM)
SMEM = pl.BlockSpec(memory_space=pltpu.SMEM)


def call(kernel, outs, scratch, name, table=True):
    def run(*args):
        specs = [VMEM] * len(args)
        if table:
            specs[0] = SMEM
        return pl.pallas_call(
            kernel,
            out_shape=outs,
            in_specs=specs,
            out_specs=jax.tree.map(lambda o: SMEM if o.dtype == jnp.int32 else VMEM, outs),
            scratch_shapes=[pltpu.VMEM(shape, F32) for shape in scratch],
            compiler_params=pltpu.CompilerParams(vmem_limit_bytes=48 * 2**20),
            name=name,
        )(*args)

    return run


SQUARE = struct(D, D)
TWO = struct(2, D, D)
TILE = struct(8, HALF)
COUNT = jax.ShapeDtypeStruct((1,), jnp.int32)
pair = call(pair_kernel, (SQUARE, SQUARE), [(4, D, D)], "pair")
window = call(window_kernel, (TWO, SQUARE), [(11, D, D)], "window")
entry = call(entry_kernel, SQUARE, [(4, D, D)], "entry")
solve = call(
    solve_kernel,
    (TWO, TWO, TWO, COUNT, COUNT),
    [(D, D)] * 4 + [(2, 2, D, D), (2, D, D)],
    "solve",
)
gauge = call(gauge_kernel, TILE, [(2, D, D), (2, D, D)], "gauge")


highest = lax.Precision.HIGHEST


def product(left, right):
    return jnp.matmul(left, right, precision=highest, preferred_element_type=F32)


def flip(value):
    return jnp.swapaxes(value, -1, -2)


def orthonormal(panel):
    def turn(t, y):
        gram = product(flip(y), y)
        mean = jnp.trace(gram, axis1=-2, axis2=-1)[:, None, None] / D
        gram = gram + jnp.where(t == 0, 1.0e-5, 0.0) * mean * jnp.eye(D, dtype=F32)
        lower = jnp.linalg.cholesky(gram)
        return flip(lax.linalg.triangular_solve(lower, flip(y), left_side=True, lower=True))

    return lax.fori_loop(0, 3, turn, panel)


def one_block(before, coupling, diagonal):
    def half(t, carried):
        panel, q = carried
        panel = jnp.where(t == 0, panel, product(coupling, q))
        return panel, orthonormal(panel)

    panel, q = lax.fori_loop(0, 2, half, (before, before))
    new = product(product(flip(q), diagonal), q)
    return new, jnp.triu(product(flip(q), panel)), q


def x_move(value, to):
    return lax.ppermute(value, "row", [(i, (i // 4) * 4 + to(i % 4)) for i in range(16)])


def z_move(value, s):
    return lax.ppermute(value, "row", [(i, i + 4 * s) for i in range(16 - 4 * s)])


def z_ring(value, s):
    return lax.ppermute(value, "row", [(i, (i + 4 * s) % 16) for i in range(16)])


def x_pairs(value):
    return x_move(value, lambda x: x ^ 1)


def x_mirror(value):
    return x_move(value, lambda x: 3 - x)


def largest(value, moves):
    return functools.reduce(jnp.maximum, moves, value)


def shards(diag_blocks, coupling_blocks):
    diagonal = diag_blocks.reshape(2, D, D)
    coupling = coupling_blocks.reshape(2, D, D)
    position = lax.axis_index("row")
    z, x = position // 4, position % 4
    mine = jnp.where((x == 0) | (x == 3), 1, 0)
    pos = jnp.stack([z, x, mine, position]).astype(jnp.int32)
    table = jnp.asarray(TABLE, jnp.int32)[x]

    r0, r1 = x_pairs(coupling[0]), x_mirror(coupling[1])
    w, v = pair(pos, coupling, r0, r1)
    q0, q1 = x_mirror(w), x_pairs(v)
    prev, total = window(table, coupling, r0, r1, w, q0, q1)
    below = [z_move(total, s) for s in (1, 2, 3)]
    gauged = gauge(pos, prev, coupling)
    gauged = largest(gauged, [x_move(gauged, lambda x, s=s: (x + s) % 4) for s in (1, 2, 3)])
    gauged, *below = lax.optimization_barrier((gauged, *below))
    own = entry(pos, *below)
    gauged, own = lax.optimization_barrier((gauged, own))
    other = x_pairs(own)
    bound = largest(gauged, [z_ring(gauged, s) for s in (1, 2, 3)])
    new, tri, before, trips, whole = solve(
        pos, prev, own, other, coupling, diagonal, bound
    )
    whole = whole.reshape(()) > 0

    def step(i, carried):
        q, new, tri = carried
        q = jnp.where(whole & (i == 0), jnp.eye(D, dtype=F32), q)
        new_now, tri_now, q = one_block(q, coupling, diagonal)
        keep = (i == position) | jnp.logical_not(whole)
        new = jnp.where(keep, new_now, new)
        tri = jnp.where(keep, tri_now, tri)
        q = lax.cond(
            whole,
            lambda q: lax.ppermute(q, "row", [(j, j + 1) for j in range(15)]),
            lambda q: q,
            q,
        )
        return q, new, tri

    _, new, tri = lax.fori_loop(0, trips.reshape(()), step, (before, new, tri))
    shape = diag_blocks.shape
    return new.reshape(shape), tri.reshape(shape)


def solution(mesh):
    placed = P("section", None, "row", None, None)
    return jax.shard_map(
        shards,
        mesh=mesh,
        in_specs=(placed, placed),
        out_specs=(placed, placed),
        check_vma=False,
    )
```

```python
import functools

import jax
import jax.numpy as jnp
from jax import lax
from jax.experimental import pallas as pl
from jax.experimental.pallas import tpu as pltpu
from jax.sharding import PartitionSpec as P

D = 256
B = 16
HALF = 128
SOLVE = 3
GRAM = 6
F32 = jnp.float32
BF16 = jnp.bfloat16
LIMIT = 16.59
ORTHO2 = 4.0e-4


def dg(a, b, ca, cb):
    return lax.dot_general(a, b, (((ca,), (cb,)), ((), ())), preferred_element_type=F32)


def split2(x):
    h = x.astype(BF16)
    return h, (x - h.astype(F32)).astype(BF16)


def split3(x):
    h = x.astype(BF16)
    r = x - h.astype(F32)
    m = r.astype(BF16)
    return h, m, (r - m.astype(F32)).astype(BF16)


def mm(a, b, ca=1, cb=0, passes=6):
    if passes == 1:
        return dg(a.astype(BF16), b.astype(BF16), ca, cb)
    if passes == 3:
        ah, al = split2(a)
        bh, bl = split2(b)
        return dg(al, bh, ca, cb) + dg(ah, bl, ca, cb) + dg(ah, bh, ca, cb)
    ah, am, al = split3(a)
    bh, bm, bl = split3(b)
    small = dg(al, bh, ca, cb) + dg(ah, bl, ca, cb) + dg(am, bm, ca, cb)
    return (small + (dg(am, bh, ca, cb) + dg(ah, bm, ca, cb))) + dg(ah, bh, ca, cb)


def square_iota():
    return (
        lax.broadcasted_iota(jnp.int32, (D, D), 0),
        lax.broadcasted_iota(jnp.int32, (D, D), 1),
    )


def pick(value, lanes):
    return jnp.take_along_axis(value, lanes, axis=1)


def row_of(value, r):
    return jnp.broadcast_to(value[r : r + 1, :], (8, HALF))


def chol_inv(refs):
    nb = len(refs)
    row = lax.broadcasted_iota(jnp.int32, (8, HALF), 0)
    lane = lax.broadcasted_iota(jnp.int32, (8, HALF), 1)
    for h in range(2):
        n0 = h * HALF
        rows = lax.broadcasted_iota(jnp.int32, (D - n0, HALF), 0) + n0
        lanes = lax.broadcasted_iota(jnp.int32, (D - n0, HALF), 1) + n0

        def panel(p, carry, h=h, n0=n0, rows=rows, lanes=lanes):
            j = pl.multiple_of(p * B, B)
            k = pl.multiple_of(n0 + p * B, B)
            first = (lane >= j) & (lane < j + 8)
            second = (lane >= j + 8) & (lane < j + B)
            unit = jnp.where(lane - j == row, 1.0, 0.0)
            unit2 = jnp.where(lane - j - 8 == row, 1.0, 0.0)
            at = [jnp.full((8, HALF), j + c, jnp.int32) for c in range(B)]
            own = (rows >= k + B) & (lanes >= k) & (lanes < k + B)
            later = lax.broadcasted_iota(jnp.int32, (B, D - n0), 1) >= j + B
            tops = [[a[pl.ds(k, 8), i * HALF : (i + 1) * HALF] for i in range(2)] for a in refs]
            bots = [[a[pl.ds(k + 8, 8), i * HALF : (i + 1) * HALF] for i in range(2)] for a in refs]
            ats = [pick(t[h], at[c]) for c in range(8) for t in tops]
            cts = [ats[n::nb] for n in range(nb)]
            ats = [pick(t[h], at[c]) for c in range(8) for t in bots]
            cbs = [ats[n::nb] for n in range(nb)]
            pts = [jnp.ones((8, HALF), F32) for _ in range(nb)]
            pbs = [jnp.ones((8, HALF), F32) for _ in range(nb)]
            for n in range(nb):
                tops[n][h] = jnp.where(first, unit, tops[n][h])
                bots[n][h] = jnp.where(first, 0.0, bots[n][h])
            for r in range(8):
                for n in range(nb):
                    top, bot, ct, cb = tops[n], bots[n], cts[n], cbs[n]
                    piv = row_of(ct[r], r)
                    inv = 1.0 / piv
                    pts[n] = jnp.where(row == r, piv, pts[n])
                    lt = jnp.where(row > r, ct[r] * inv, 0.0)
                    lb = cb[r] * inv
                    for c in range(r + 1, 8):
                        u = row_of(ct[c], r)
                        ct[c] = ct[c] - lt * u
                        cb[c] = cb[c] - lb * u
                    for i in range(2):
                        u = row_of(top[i], r)
                        if r < 7:
                            top[i] = top[i] - lt * u
                        bot[i] = bot[i] - lb * u
            ats = [pick(t[h], at[8 + c]) for c in range(8) for t in bots]
            cts = [ats[n::nb] for n in range(nb)]
            for n in range(nb):
                tops[n][h] = jnp.where(second, 0.0, tops[n][h])
                bots[n][h] = jnp.where(second, unit2, bots[n][h])
            for r in range(8):
                for n in range(nb):
                    bot, ct = bots[n], cts[n]
                    piv = row_of(ct[r], r)
                    pbs[n] = jnp.where(row == r, piv, pbs[n])
                    if r == 7:
                        continue
                    lb = jnp.where(row > r, ct[r] * (1.0 / piv), 0.0)
                    for c in range(r + 1, 8):
                        ct[c] = ct[c] - lb * row_of(ct[c], r)
                    for i in range(2):
                        bot[i] = bot[i] - lb * row_of(bot[i], r)
            scaled = []
            for n in range(nb):
                rt = lax.rsqrt(pts[n])
                rb = lax.rsqrt(pbs[n])
                scaled.append(
                    jnp.concatenate(
                        [
                            jnp.concatenate([tops[n][0] * rt, tops[n][1] * rt], 1),
                            jnp.concatenate([bots[n][0] * rb, bots[n][1] * rb], 1),
                        ],
                        0,
                    )
                )
            updates = []
            for n in range(nb):
                hi, md, lo = split3(scaled[n])
                right = jnp.concatenate([hi, lo, md, hi, md, hi], 0)
                hi, md, lo = split3(jnp.where(later, scaled[n][:, n0:], 0.0))
                left = jnp.concatenate([lo, hi, md, md, hi, hi], 0)
                updates.append(dg(left, right, 0, 0))
            for n in range(nb):
                for i in range(2):
                    old = refs[n][n0:, i * HALF : (i + 1) * HALF]
                    kept = jnp.where(own, 0.0, old) if i == h else old
                    refs[n][n0:, i * HALF : (i + 1) * HALF] = (
                        kept - updates[n][:, i * HALF : (i + 1) * HALF]
                    )
                refs[n][pl.ds(k, B), :] = scaled[n]
            return carry

        lax.fori_loop(0, HALF // B, panel, 0)


TABLE = (
    (6, 1, 3, 8, 0, 0, 2, 7, 7, 9),
    (5, 4, 0, 0, 0, 0, 1, 2, 6, 8),
    (4, 5, 3, 6, 0, 0, 2, 5, 9, 8),
    (6, 3, 1, 8, 2, 5, 3, 10, 8, 9),
)


def eye_value():
    r, c = square_iota()
    return jnp.where(r == c, 1.0, 0.0)


def pair_kernel(pos_ref, c_ref, r0, r1, w_ref, v_ref, buf):
    x = pos_ref[1]
    odd = lax.rem(x, 2)
    high = x // 2
    buf[odd] = c_ref[0]
    buf[1 - odd] = r0[...]
    buf[2 + high] = c_ref[1]
    buf[3 - high] = r1[...]
    w_ref[...] = mm(buf[1], buf[0])
    outer = (x == 0) | (x == 3)

    @pl.when(outer)
    def _():
        v_ref[...] = buf[2]

    @pl.when(jnp.logical_not(outer))
    def _():
        v_ref[...] = mm(buf[3], buf[2])


def window_kernel(tab_ref, c_ref, r0, r1, w, q0, q1, prev_ref, t_ref, buf):
    buf[0] = c_ref[0]
    buf[1] = c_ref[1]
    for k, ref in enumerate((r0, r1, w, q0, q1)):
        buf[2 + k] = ref[...]
    buf[7] = eye_value()

    def step(i, _):
        buf[8 + i] = mm(buf[tab_ref[2 * i]], buf[tab_ref[2 * i + 1]])
        return 0

    lax.fori_loop(0, tab_ref[6], step, 0)
    prev_ref[0] = buf[tab_ref[7]]
    prev_ref[1] = buf[tab_ref[8]]
    t_ref[...] = buf[tab_ref[9]]


def entry_kernel(pos_ref, t1, t2, t3, e_ref, buf):
    z = pos_ref[0]
    buf[0] = eye_value()
    for k, ref in enumerate((t1, t2, t3)):
        buf[1 + k] = ref[...]
    e_ref[...] = buf[z]

    def step(i, _):
        e_ref[...] = mm(buf[z - 1 - i], e_ref[...])
        return 0

    lax.fori_loop(0, z - 1, step, 0)


def refinement(y, passes):
    r, c = square_iota()
    err = mm(y, y, 0, 0, passes=3) - jnp.where(r == c, 1.0, 0.0)
    upper = jnp.where(c > r, err, jnp.where(c == r, 0.5 * err, 0.0))
    return mm(y, upper, passes=passes), err


def total_of(value):
    return jnp.sum(jnp.sum(value, axis=0, keepdims=True), axis=1, keepdims=True)


def solve_kernel(
    pos_ref,
    prev_ref,
    own,
    other,
    c_ref,
    d_ref,
    bound_ref,
    n_ref,
    r_ref,
    before_ref,
    trips_ref,
    whole_ref,
    *scratch,
):
    refs, m_ref, now = scratch[:4], scratch[4], scratch[5]
    mine = pos_ref[2]
    now[mine] = own[...]
    now[1 - mine] = other[...]

    def products(t, carry):
        left = [jnp.where(t == 0, prev_ref[m], c_ref[m]) for m in range(2)]
        out = [mm(left[m], now[m]) for m in range(2)]
        for m in range(2):
            now[m] = out[m]
            m_ref[t, m] = out[m]
        return carry

    lax.fori_loop(0, 2, products, 0)
    for m in range(2):
        before_ref[m] = m_ref[0, m]

    def grams(t, carry):
        out = [mm(m_ref[t, m], m_ref[t, m], 0, 0, passes=GRAM) for m in range(2)]
        for m in range(2):
            now[m] = out[m]

        @pl.when(t == 0)
        def _():
            for m in range(2):
                refs[m][...] = now[m]

        @pl.when(t == 1)
        def _():
            for m in range(2):
                refs[2 + m][...] = now[m]

        return carry

    lax.fori_loop(0, 2, grams, 0)
    chol_inv(refs)
    r, c = square_iota()

    def factors(t, worst):
        inv = [
            jnp.where(c <= r, jnp.where(t == 0, refs[m][...], refs[2 + m][...]), 0.0)
            for m in range(2)
        ]
        ys = [mm(m_ref[t, m], inv[m], 1, 1) for m in range(2)]
        for m in range(2):
            change, err = refinement(ys[m], 1)
            m_ref[t, m] = ys[m] - change
            worst = jnp.maximum(worst, jnp.where(total_of(err * err) < ORTHO2, 0.0, 1.0))
        return worst

    worst = lax.fori_loop(0, 2, factors, jnp.zeros((1, 1), F32))
    fine = bound_of(bound_ref[...]) < LIMIT
    trips_ref[0] = jnp.where(fine, jnp.where(worst[0, 0] > 0.0, 1, 0), 16)
    whole_ref[0] = jnp.where(fine, 0, 1)

    def results(t, carry):
        left = [jnp.where(t == 0, c_ref[m], d_ref[m]) for m in range(2)]
        part = [mm(left[m], m_ref[t, m], passes=SOLVE) for m in range(2)]
        out = [mm(m_ref[1, m], part[m], 0, 0, passes=SOLVE) for m in range(2)]
        for m in range(2):
            now[m] = out[m]

        @pl.when(t == 0)
        def _():
            for m in range(2):
                r_ref[m] = jnp.where(c >= r, now[m], 0.0)

        @pl.when(t == 1)
        def _():
            for m in range(2):
                n_ref[m] = now[m]

        return carry

    lax.fori_loop(0, 2, results, 0)


def gauge_kernel(pos_ref, prev_ref, c_ref, out_ref, g_ref, b_ref):
    eye = eye_value()
    row = lax.broadcasted_iota(jnp.int32, (8, HALF), 0)
    lane = lax.broadcasted_iota(jnp.int32, (8, HALF), 1)
    norms = []
    for m in range(2):
        full = mm(c_ref[m], prev_ref[m], passes=3)
        gram = mm(full, full, 0, 0, passes=3)
        norm = jnp.sqrt(total_of(gram * gram))
        g_ref[m] = gram / norm
    for m in range(2):
        b_ref[m] = mm(g_ref[m], g_ref[m], passes=3)
    for _ in range(3):
        for m in range(2):
            b_ref[m] = mm(b_ref[m], b_ref[m], passes=3)
    for m in range(2):
        top = jnp.exp(0.0625 * 0.5 * jnp.log(total_of(b_ref[m] * b_ref[m]))) * 1.02
        b_ref[m] = eye - g_ref[m] / top
    for t in range(10):
        for m in range(2):
            b_ref[m] = mm(b_ref[m], b_ref[m], passes=3 if t < 5 else 1)
    out = jnp.zeros((8, HALF), F32)
    for m in range(2):
        norm = jnp.maximum(total_of(b_ref[m] * b_ref[m]), 1.0e-30)
        low = jnp.maximum(1.0 - jnp.exp(jnp.log(norm) / 2048.0), 1.0e-9)
        value = jnp.broadcast_to(-jnp.log(low), (8, HALF))
        out = jnp.where((row == m) & (lane == pos_ref[3]), value, out)
    out_ref[...] = out


def bound_of(v):
    lane = lax.broadcasted_iota(jnp.int32, (8, HALF), 1)
    bound = v
    for z in range(3):
        whole = jnp.sum(jnp.where(lane == 4 * z + 3, v, 0.0), axis=1, keepdims=True)
        bound = bound + jnp.where(lane >= 4 * z + 4, whole, 0.0)
    bound = jnp.where(lane < 16, bound, 0.0)
    return jnp.max(jnp.max(bound, axis=0, keepdims=True), axis=1, keepdims=True)[0, 0]


def struct(*shape):
    return jax.ShapeDtypeStruct(shape, F32)


VMEM = pl.BlockSpec(memory_space=pltpu.VMEM)
SMEM = pl.BlockSpec(memory_space=pltpu.SMEM)


def call(kernel, outs, scratch, name, table=True):
    def run(*args):
        specs = [VMEM] * len(args)
        if table:
            specs[0] = SMEM
        return pl.pallas_call(
            kernel,
            out_shape=outs,
            in_specs=specs,
            out_specs=jax.tree.map(lambda o: SMEM if o.dtype == jnp.int32 else VMEM, outs),
            scratch_shapes=[pltpu.VMEM(shape, F32) for shape in scratch],
            compiler_params=pltpu.CompilerParams(vmem_limit_bytes=48 * 2**20),
            name=name,
        )(*args)

    return run


SQUARE = struct(D, D)
TWO = struct(2, D, D)
TILE = struct(8, HALF)
COUNT = jax.ShapeDtypeStruct((1,), jnp.int32)
pair = call(pair_kernel, (SQUARE, SQUARE), [(4, D, D)], "pair")
window = call(window_kernel, (TWO, SQUARE), [(11, D, D)], "window")
entry = call(entry_kernel, SQUARE, [(4, D, D)], "entry")
solve = call(
    solve_kernel,
    (TWO, TWO, TWO, COUNT, COUNT),
    [(D, D)] * 4 + [(2, 2, D, D), (2, D, D)],
    "solve",
)
gauge = call(gauge_kernel, TILE, [(2, D, D), (2, D, D)], "gauge")


highest = lax.Precision.HIGHEST


def product(left, right):
    return jnp.matmul(left, right, precision=highest, preferred_element_type=F32)


def flip(value):
    return jnp.swapaxes(value, -1, -2)


def orthonormal(panel):
    def turn(t, y):
        gram = product(flip(y), y)
        mean = jnp.trace(gram, axis1=-2, axis2=-1)[:, None, None] / D
        gram = gram + jnp.where(t == 0, 1.0e-5, 0.0) * mean * jnp.eye(D, dtype=F32)
        lower = jnp.linalg.cholesky(gram)
        return flip(lax.linalg.triangular_solve(lower, flip(y), left_side=True, lower=True))

    return lax.fori_loop(0, 3, turn, panel)


def one_block(before, coupling, diagonal):
    def half(t, carried):
        panel, q = carried
        panel = jnp.where(t == 0, panel, product(coupling, q))
        return panel, orthonormal(panel)

    panel, q = lax.fori_loop(0, 2, half, (before, before))
    new = product(product(flip(q), diagonal), q)
    return new, jnp.triu(product(flip(q), panel)), q


def x_move(value, to):
    return lax.ppermute(value, "row", [(i, (i // 4) * 4 + to(i % 4)) for i in range(16)])


def z_move(value, s):
    return lax.ppermute(value, "row", [(i, i + 4 * s) for i in range(16 - 4 * s)])


def z_ring(value, s):
    return lax.ppermute(value, "row", [(i, (i + 4 * s) % 16) for i in range(16)])


def x_pairs(value):
    return x_move(value, lambda x: x ^ 1)


def x_mirror(value):
    return x_move(value, lambda x: 3 - x)


def largest(value, moves):
    return functools.reduce(jnp.maximum, moves, value)


def shards(diag_blocks, coupling_blocks):
    diagonal = diag_blocks.reshape(2, D, D)
    coupling = coupling_blocks.reshape(2, D, D)
    position = lax.axis_index("row")
    z, x = position // 4, position % 4
    mine = jnp.where((x == 0) | (x == 3), 1, 0)
    pos = jnp.stack([z, x, mine, position]).astype(jnp.int32)
    table = jnp.asarray(TABLE, jnp.int32)[x]

    r0, r1 = x_pairs(coupling[0]), x_mirror(coupling[1])
    w, v = pair(pos, coupling, r0, r1)
    q0, q1 = x_mirror(w), x_pairs(v)
    prev, total = window(table, coupling, r0, r1, w, q0, q1)
    below = [z_move(total, s) for s in (1, 2, 3)]
    gauged = gauge(pos, prev, coupling)
    gauged = largest(gauged, [x_move(gauged, lambda x, s=s: (x + s) % 4) for s in (1, 2, 3)])
    gauged, *below = lax.optimization_barrier((gauged, *below))
    own = entry(pos, *below)
    gauged, own = lax.optimization_barrier((gauged, own))
    other = x_pairs(own)
    bound = largest(gauged, [z_ring(gauged, s) for s in (1, 2, 3)])
    new, tri, before, trips, whole = solve(
        pos, prev, own, other, coupling, diagonal, bound
    )
    whole = whole.reshape(()) > 0

    def step(i, carried):
        q, new, tri = carried
        q = jnp.where(whole & (i == 0), jnp.eye(D, dtype=F32), q)
        new_now, tri_now, q = one_block(q, coupling, diagonal)
        keep = (i == position) | jnp.logical_not(whole)
        new = jnp.where(keep, new_now, new)
        tri = jnp.where(keep, tri_now, tri)
        q = lax.cond(
            whole,
            lambda q: lax.ppermute(q, "row", [(j, j + 1) for j in range(15)]),
            lambda q: q,
            q,
        )
        return q, new, tri

    _, new, tri = lax.fori_loop(0, trips.reshape(()), step, (before, new, tri))
    shape = diag_blocks.shape
    return new.reshape(shape), tri.reshape(shape)


def solution(mesh):
    placed = P("section", None, "row", None, None)
    return jax.shard_map(
        shards,
        mesh=mesh,
        in_specs=(placed, placed),
        out_specs=(placed, placed),
        check_vma=False,
    )
```

```python
import functools

import jax
import jax.numpy as jnp
from jax import lax
from jax.experimental import pallas as pl
from jax.experimental.pallas import tpu as pltpu
from jax.sharding import PartitionSpec as P

D = 256
B = 16
HALF = 128
SOLVE = 3
GRAM = 6
F32 = jnp.float32
BF16 = jnp.bfloat16
LIMIT = 16.59
ORTHO2 = 4.0e-4


def dg(a, b, ca, cb):
    return lax.dot_general(a, b, (((ca,), (cb,)), ((), ())), preferred_element_type=F32)


def split2(x):
    h = x.astype(BF16)
    return h, (x - h.astype(F32)).astype(BF16)


def split3(x):
    h = x.astype(BF16)
    r = x - h.astype(F32)
    m = r.astype(BF16)
    return h, m, (r - m.astype(F32)).astype(BF16)


def mm(a, b, ca=1, cb=0, passes=6):
    if passes == 1:
        return dg(a.astype(BF16), b.astype(BF16), ca, cb)
    if passes == 3:
        ah, al = split2(a)
        bh, bl = split2(b)
        return dg(al, bh, ca, cb) + dg(ah, bl, ca, cb) + dg(ah, bh, ca, cb)
    ah, am, al = split3(a)
    bh, bm, bl = split3(b)
    small = dg(al, bh, ca, cb) + dg(ah, bl, ca, cb) + dg(am, bm, ca, cb)
    return (small + (dg(am, bh, ca, cb) + dg(ah, bm, ca, cb))) + dg(ah, bh, ca, cb)


def square_iota():
    return (
        lax.broadcasted_iota(jnp.int32, (D, D), 0),
        lax.broadcasted_iota(jnp.int32, (D, D), 1),
    )


def pick(value, lanes):
    return jnp.take_along_axis(value, lanes, axis=1)


def row_of(value, r):
    return jnp.broadcast_to(value[r : r + 1, :], (8, HALF))


def chol_inv(refs):
    nb = len(refs)
    row = lax.broadcasted_iota(jnp.int32, (8, HALF), 0)
    lane = lax.broadcasted_iota(jnp.int32, (8, HALF), 1)
    for h in range(2):
        n0 = h * HALF
        rows = lax.broadcasted_iota(jnp.int32, (D - n0, HALF), 0) + n0
        lanes = lax.broadcasted_iota(jnp.int32, (D - n0, HALF), 1) + n0

        def panel(p, carry, h=h, n0=n0, rows=rows, lanes=lanes):
            j = pl.multiple_of(p * B, B)
            k = pl.multiple_of(n0 + p * B, B)
            first = (lane >= j) & (lane < j + 8)
            second = (lane >= j + 8) & (lane < j + B)
            unit = jnp.where(lane - j == row, 1.0, 0.0)
            unit2 = jnp.where(lane - j - 8 == row, 1.0, 0.0)
            at = [jnp.full((8, HALF), j + c, jnp.int32) for c in range(B)]
            own = (rows >= k + B) & (lanes >= k) & (lanes < k + B)
            later = lax.broadcasted_iota(jnp.int32, (B, D - n0), 1) >= j + B
            tops = [[a[pl.ds(k, 8), i * HALF : (i + 1) * HALF] for i in range(2)] for a in refs]
            bots = [[a[pl.ds(k + 8, 8), i * HALF : (i + 1) * HALF] for i in range(2)] for a in refs]
            ats = [pick(t[h], at[c]) for c in range(8) for t in tops]
            cts = [ats[n::nb] for n in range(nb)]
            ats = [pick(t[h], at[c]) for c in range(8) for t in bots]
            cbs = [ats[n::nb] for n in range(nb)]
            pts = [jnp.ones((8, HALF), F32) for _ in range(nb)]
            pbs = [jnp.ones((8, HALF), F32) for _ in range(nb)]
            for n in range(nb):
                tops[n][h] = jnp.where(first, unit, tops[n][h])
                bots[n][h] = jnp.where(first, 0.0, bots[n][h])
            for r in range(8):
                for n in range(nb):
                    top, bot, ct, cb = tops[n], bots[n], cts[n], cbs[n]
                    piv = row_of(ct[r], r)
                    inv = 1.0 / piv
                    pts[n] = jnp.where(row == r, piv, pts[n])
                    lt = jnp.where(row > r, ct[r] * inv, 0.0)
                    lb = cb[r] * inv
                    for c in range(r + 1, 8):
                        u = row_of(ct[c], r)
                        ct[c] = ct[c] - lt * u
                        cb[c] = cb[c] - lb * u
                    for i in range(2):
                        u = row_of(top[i], r)
                        if r < 7:
                            top[i] = top[i] - lt * u
                        bot[i] = bot[i] - lb * u
            ats = [pick(t[h], at[8 + c]) for c in range(8) for t in bots]
            cts = [ats[n::nb] for n in range(nb)]
            for n in range(nb):
                tops[n][h] = jnp.where(second, 0.0, tops[n][h])
                bots[n][h] = jnp.where(second, unit2, bots[n][h])
            for r in range(8):
                for n in range(nb):
                    bot, ct = bots[n], cts[n]
                    piv = row_of(ct[r], r)
                    pbs[n] = jnp.where(row == r, piv, pbs[n])
                    if r == 7:
                        continue
                    lb = jnp.where(row > r, ct[r] * (1.0 / piv), 0.0)
                    for c in range(r + 1, 8):
                        ct[c] = ct[c] - lb * row_of(ct[c], r)
                    for i in range(2):
                        bot[i] = bot[i] - lb * row_of(bot[i], r)
            scaled = []
            for n in range(nb):
                rt = lax.rsqrt(pts[n])
                rb = lax.rsqrt(pbs[n])
                scaled.append(
                    jnp.concatenate(
                        [
                            jnp.concatenate([tops[n][0] * rt, tops[n][1] * rt], 1),
                            jnp.concatenate([bots[n][0] * rb, bots[n][1] * rb], 1),
                        ],
                        0,
                    )
                )
            updates = []
            for n in range(nb):
                hi, md, lo = split3(scaled[n])
                right = jnp.concatenate([hi, lo, md, hi, md, hi], 0)
                hi, md, lo = split3(jnp.where(later, scaled[n][:, n0:], 0.0))
                left = jnp.concatenate([lo, hi, md, md, hi, hi], 0)
                updates.append(dg(left, right, 0, 0))
            for n in range(nb):
                for i in range(2):
                    old = refs[n][n0:, i * HALF : (i + 1) * HALF]
                    kept = jnp.where(own, 0.0, old) if i == h else old
                    refs[n][n0:, i * HALF : (i + 1) * HALF] = (
                        kept - updates[n][:, i * HALF : (i + 1) * HALF]
                    )
                refs[n][pl.ds(k, B), :] = scaled[n]
            return carry

        lax.fori_loop(0, HALF // B, panel, 0)


TABLE = (
    (6, 1, 3, 8, 0, 0, 2, 7, 7, 9),
    (5, 4, 0, 0, 0, 0, 1, 2, 6, 8),
    (4, 5, 3, 6, 0, 0, 2, 5, 9, 8),
    (6, 3, 1, 8, 2, 5, 3, 10, 8, 9),
)


def eye_value():
    r, c = square_iota()
    return jnp.where(r == c, 1.0, 0.0)


def pair_kernel(pos_ref, c_ref, r0, r1, w_ref, v_ref, buf):
    x = pos_ref[1]
    odd = lax.rem(x, 2)
    high = x // 2
    buf[odd] = c_ref[0]
    buf[1 - odd] = r0[...]
    buf[2 + high] = c_ref[1]
    buf[3 - high] = r1[...]
    w = mm(buf[1], buf[0])
    v = mm(buf[3], buf[2])
    outer = (x == 0) | (x == 3)
    w_ref[...] = w
    v_ref[...] = jnp.where(outer, buf[2], v)


def window_kernel(tab_ref, c_ref, r0, r1, w, q0, q1, prev_ref, t_ref, buf):
    buf[0] = c_ref[0]
    buf[1] = c_ref[1]
    for k, ref in enumerate((r0, r1, w, q0, q1)):
        buf[2 + k] = ref[...]
    buf[7] = eye_value()

    def step(i, _):
        buf[8 + i] = mm(buf[tab_ref[2 * i]], buf[tab_ref[2 * i + 1]])
        return 0

    lax.fori_loop(0, tab_ref[6], step, 0)
    prev_ref[0] = buf[tab_ref[7]]
    prev_ref[1] = buf[tab_ref[8]]
    t_ref[...] = buf[tab_ref[9]]


def entry_kernel(pos_ref, t1, t2, t3, e_ref, buf):
    z = pos_ref[0]
    buf[0] = eye_value()
    for k, ref in enumerate((t1, t2, t3)):
        buf[1 + k] = ref[...]
    e_ref[...] = buf[z]

    def step(i, _):
        e_ref[...] = mm(buf[z - 1 - i], e_ref[...])
        return 0

    lax.fori_loop(0, z - 1, step, 0)


def refinement(y, passes):
    r, c = square_iota()
    err = mm(y, y, 0, 0, passes=3) - jnp.where(r == c, 1.0, 0.0)
    upper = jnp.where(c > r, err, jnp.where(c == r, 0.5 * err, 0.0))
    return mm(y, upper, passes=passes), err


def total_of(value):
    return jnp.sum(jnp.sum(value, axis=0, keepdims=True), axis=1, keepdims=True)


def head_kernel(pos_ref, prev_ref, own, c_ref, head_ref, gram_ref):
    mine = pos_ref[2]
    before = mm(prev_ref[mine], own[...])
    after = mm(c_ref[mine], before)
    head_ref[0] = before
    head_ref[1] = after
    gram_ref[0] = mm(before, before, 0, 0, passes=GRAM)
    gram_ref[1] = mm(after, after, 0, 0, passes=GRAM)


def solve_kernel(
    pos_ref,
    prev_ref,
    head_ref,
    gram_ref,
    other,
    c_ref,
    d_ref,
    bound_ref,
    n_ref,
    r_ref,
    before_ref,
    trips_ref,
    whole_ref,
    *scratch,
):
    refs, m_ref, now = scratch[:4], scratch[4], scratch[5]
    slots = (pos_ref[2], 1 - pos_ref[2])
    rest = slots[1]
    before = mm(prev_ref[rest], other[...])
    after = mm(c_ref[rest], before)
    m_ref[0, 0] = head_ref[0]
    m_ref[1, 0] = head_ref[1]
    m_ref[0, 1] = before
    m_ref[1, 1] = after
    refs[0][...] = gram_ref[0]
    refs[2][...] = gram_ref[1]
    refs[1][...] = mm(before, before, 0, 0, passes=GRAM)
    refs[3][...] = mm(after, after, 0, 0, passes=GRAM)
    for n, m in enumerate(slots):
        before_ref[m] = m_ref[0, n]
    chol_inv(refs)
    r, c = square_iota()

    def factors(t, worst):
        inv = [
            jnp.where(c <= r, jnp.where(t == 0, refs[m][...], refs[2 + m][...]), 0.0)
            for m in range(2)
        ]
        ys = [mm(m_ref[t, m], inv[m], 1, 1) for m in range(2)]
        for m in range(2):
            change, err = refinement(ys[m], 1)
            m_ref[t, m] = ys[m] - change
            worst = jnp.maximum(worst, jnp.where(total_of(err * err) < ORTHO2, 0.0, 1.0))
        return worst

    worst = lax.fori_loop(0, 2, factors, jnp.zeros((1, 1), F32))
    fine = bound_of(bound_ref[...]) < LIMIT
    trips_ref[0] = jnp.where(fine, jnp.where(worst[0, 0] > 0.0, 1, 0), 16)
    whole_ref[0] = jnp.where(fine, 0, 1)

    def results(t, carry):
        left = [jnp.where(t == 0, c_ref[m], d_ref[m]) for m in slots]
        part = [mm(left[m], m_ref[t, m], passes=SOLVE) for m in range(2)]
        out = [mm(m_ref[1, m], part[m], 0, 0, passes=SOLVE) for m in range(2)]
        for m in range(2):
            now[m] = out[m]

        @pl.when(t == 0)
        def _():
            for n, m in enumerate(slots):
                r_ref[m] = jnp.where(c >= r, now[n], 0.0)

        @pl.when(t == 1)
        def _():
            for n, m in enumerate(slots):
                n_ref[m] = now[n]

        return carry

    lax.fori_loop(0, 2, results, 0)


def gauge_kernel(pos_ref, prev_ref, c_ref, out_ref, g_ref, b_ref):
    eye = eye_value()
    row = lax.broadcasted_iota(jnp.int32, (8, HALF), 0)
    lane = lax.broadcasted_iota(jnp.int32, (8, HALF), 1)
    norms = []
    for m in range(2):
        full = mm(c_ref[m], prev_ref[m], passes=3)
        gram = mm(full, full, 0, 0, passes=3)
        norm = jnp.sqrt(total_of(gram * gram))
        g_ref[m] = gram / norm
    for m in range(2):
        b_ref[m] = mm(g_ref[m], g_ref[m], passes=3)
    for _ in range(3):
        for m in range(2):
            b_ref[m] = mm(b_ref[m], b_ref[m], passes=3)
    for m in range(2):
        top = jnp.exp(0.0625 * 0.5 * jnp.log(total_of(b_ref[m] * b_ref[m]))) * 1.02
        b_ref[m] = eye - g_ref[m] / top
    for t in range(10):
        for m in range(2):
            b_ref[m] = mm(b_ref[m], b_ref[m], passes=3 if t < 5 else 1)
    out = jnp.zeros((8, HALF), F32)
    for m in range(2):
        norm = jnp.maximum(total_of(b_ref[m] * b_ref[m]), 1.0e-30)
        low = jnp.maximum(1.0 - jnp.exp(jnp.log(norm) / 2048.0), 1.0e-9)
        value = jnp.broadcast_to(-jnp.log(low), (8, HALF))
        out = jnp.where((row == m) & (lane == pos_ref[3]), value, out)
    out_ref[...] = out


def bound_of(v):
    lane = lax.broadcasted_iota(jnp.int32, (8, HALF), 1)
    bound = v
    for z in range(3):
        whole = jnp.sum(jnp.where(lane == 4 * z + 3, v, 0.0), axis=1, keepdims=True)
        bound = bound + jnp.where(lane >= 4 * z + 4, whole, 0.0)
    bound = jnp.where(lane < 16, bound, 0.0)
    return jnp.max(jnp.max(bound, axis=0, keepdims=True), axis=1, keepdims=True)[0, 0]


def struct(*shape):
    return jax.ShapeDtypeStruct(shape, F32)


VMEM = pl.BlockSpec(memory_space=pltpu.VMEM)
SMEM = pl.BlockSpec(memory_space=pltpu.SMEM)


def call(kernel, outs, scratch, name, table=True):
    def run(*args):
        specs = [VMEM] * len(args)
        if table:
            specs[0] = SMEM
        return pl.pallas_call(
            kernel,
            out_shape=outs,
            in_specs=specs,
            out_specs=jax.tree.map(lambda o: SMEM if o.dtype == jnp.int32 else VMEM, outs),
            scratch_shapes=[pltpu.VMEM(shape, F32) for shape in scratch],
            compiler_params=pltpu.CompilerParams(vmem_limit_bytes=48 * 2**20),
            name=name,
        )(*args)

    return run


SQUARE = struct(D, D)
TWO = struct(2, D, D)
TILE = struct(8, HALF)
COUNT = jax.ShapeDtypeStruct((1,), jnp.int32)
pair = call(pair_kernel, (SQUARE, SQUARE), [(4, D, D)], "pair")
window = call(window_kernel, (TWO, SQUARE), [(11, D, D)], "window")
entry = call(entry_kernel, SQUARE, [(4, D, D)], "entry")
solve = call(
    solve_kernel,
    (TWO, TWO, TWO, COUNT, COUNT),
    [(D, D)] * 4 + [(2, 2, D, D), (2, D, D)],
    "solve",
)
head = call(head_kernel, (TWO, TWO), [], "head")
gauge = call(gauge_kernel, TILE, [(2, D, D), (2, D, D)], "gauge")


highest = lax.Precision.HIGHEST


def product(left, right):
    return jnp.matmul(left, right, precision=highest, preferred_element_type=F32)


def flip(value):
    return jnp.swapaxes(value, -1, -2)


def orthonormal(panel):
    def turn(t, y):
        gram = product(flip(y), y)
        mean = jnp.trace(gram, axis1=-2, axis2=-1)[:, None, None] / D
        gram = gram + jnp.where(t == 0, 1.0e-5, 0.0) * mean * jnp.eye(D, dtype=F32)
        lower = jnp.linalg.cholesky(gram)
        return flip(lax.linalg.triangular_solve(lower, flip(y), left_side=True, lower=True))

    return lax.fori_loop(0, 3, turn, panel)


def one_block(before, coupling, diagonal):
    def half(t, carried):
        panel, q = carried
        panel = jnp.where(t == 0, panel, product(coupling, q))
        return panel, orthonormal(panel)

    panel, q = lax.fori_loop(0, 2, half, (before, before))
    new = product(product(flip(q), diagonal), q)
    return new, jnp.triu(product(flip(q), panel)), q


def x_move(value, to):
    return lax.ppermute(value, "row", [(i, (i // 4) * 4 + to(i % 4)) for i in range(16)])


def z_move(value, s):
    return lax.ppermute(value, "row", [(i, i + 4 * s) for i in range(16 - 4 * s)])


def z_ring(value, s):
    return lax.ppermute(value, "row", [(i, (i + 4 * s) % 16) for i in range(16)])


def x_pairs(value):
    return x_move(value, lambda x: x ^ 1)


def x_mirror(value):
    return x_move(value, lambda x: 3 - x)


def largest(value, moves):
    return functools.reduce(jnp.maximum, moves, value)


def shards(diag_blocks, coupling_blocks):
    diagonal = diag_blocks.reshape(2, D, D)
    coupling = coupling_blocks.reshape(2, D, D)
    position = lax.axis_index("row")
    z, x = position // 4, position % 4
    mine = jnp.where((x == 0) | (x == 3), 1, 0)
    pos = jnp.stack([z, x, mine, position]).astype(jnp.int32)
    table = jnp.asarray(TABLE, jnp.int32)[x]

    r0, r1 = x_pairs(coupling[0]), x_mirror(coupling[1])
    w, v = pair(pos, coupling, r0, r1)
    q0, q1 = x_mirror(w), x_pairs(v)
    prev, total = window(table, coupling, r0, r1, w, q0, q1)
    below = [z_move(total, s) for s in (1, 2, 3)]
    gauged = gauge(pos, prev, coupling)
    gauged = largest(gauged, [x_move(gauged, lambda x, s=s: (x + s) % 4) for s in (1, 2, 3)])
    gauged, *below = lax.optimization_barrier((gauged, *below))
    own = entry(pos, *below)
    gauged, own = lax.optimization_barrier((gauged, own))
    other = x_pairs(own)
    bound = largest(gauged, [z_ring(gauged, s) for s in (1, 2, 3)])
    new, tri, before, trips, whole = solve(
        pos, prev, *head(pos, prev, own, coupling), other, coupling, diagonal, bound
    )
    whole = whole.reshape(()) > 0

    def step(i, carried):
        q, new, tri = carried
        q = jnp.where(whole & (i == 0), jnp.eye(D, dtype=F32), q)
        new_now, tri_now, q = one_block(q, coupling, diagonal)
        keep = (i == position) | jnp.logical_not(whole)
        new = jnp.where(keep, new_now, new)
        tri = jnp.where(keep, tri_now, tri)
        q = lax.cond(
            whole,
            lambda q: lax.ppermute(q, "row", [(j, j + 1) for j in range(15)]),
            lambda q: q,
            q,
        )
        return q, new, tri

    _, new, tri = lax.fori_loop(0, trips.reshape(()), step, (before, new, tri))
    shape = diag_blocks.shape
    return new.reshape(shape), tri.reshape(shape)


def solution(mesh):
    placed = P("section", None, "row", None, None)
    return jax.shard_map(
        shards,
        mesh=mesh,
        in_specs=(placed, placed),
        out_specs=(placed, placed),
        check_vma=False,
    )
```

```python
import functools

import jax
import jax.numpy as jnp
from jax import lax
from jax.experimental import pallas as pl
from jax.experimental.pallas import tpu as pltpu
from jax.sharding import PartitionSpec as P

D = 256
B = 16
HALF = 128
SOLVE = 3
GRAM = 6
F32 = jnp.float32
BF16 = jnp.bfloat16
LIMIT = 16.59
ORTHO2 = 4.0e-4


def dg(a, b, ca, cb):
    return lax.dot_general(a, b, (((ca,), (cb,)), ((), ())), preferred_element_type=F32)


def split2(x):
    h = x.astype(BF16)
    return h, (x - h.astype(F32)).astype(BF16)


def split3(x):
    h = x.astype(BF16)
    r = x - h.astype(F32)
    m = r.astype(BF16)
    return h, m, (r - m.astype(F32)).astype(BF16)


def mm(a, b, ca=1, cb=0, passes=6):
    if passes == 1:
        return dg(a.astype(BF16), b.astype(BF16), ca, cb)
    if passes == 3:
        ah, al = split2(a)
        bh, bl = split2(b)
        return dg(al, bh, ca, cb) + dg(ah, bl, ca, cb) + dg(ah, bh, ca, cb)
    ah, am, al = split3(a)
    bh, bm, bl = split3(b)
    small = dg(al, bh, ca, cb) + dg(ah, bl, ca, cb) + dg(am, bm, ca, cb)
    return (small + (dg(am, bh, ca, cb) + dg(ah, bm, ca, cb))) + dg(ah, bh, ca, cb)


def square_iota():
    return (
        lax.broadcasted_iota(jnp.int32, (D, D), 0),
        lax.broadcasted_iota(jnp.int32, (D, D), 1),
    )


def pick(value, lanes):
    return jnp.take_along_axis(value, lanes, axis=1)


def row_of(value, r):
    return jnp.broadcast_to(value[r : r + 1, :], (8, HALF))


def chol_inv(refs):
    nb = len(refs)
    row = lax.broadcasted_iota(jnp.int32, (8, HALF), 0)
    lane = lax.broadcasted_iota(jnp.int32, (8, HALF), 1)
    for h in range(2):
        n0 = h * HALF
        rows = lax.broadcasted_iota(jnp.int32, (D - n0, HALF), 0) + n0
        lanes = lax.broadcasted_iota(jnp.int32, (D - n0, HALF), 1) + n0

        def panel(p, carry, h=h, n0=n0, rows=rows, lanes=lanes):
            j = pl.multiple_of(p * B, B)
            k = pl.multiple_of(n0 + p * B, B)
            first = (lane >= j) & (lane < j + 8)
            second = (lane >= j + 8) & (lane < j + B)
            unit = jnp.where(lane - j == row, 1.0, 0.0)
            unit2 = jnp.where(lane - j - 8 == row, 1.0, 0.0)
            at = [jnp.full((8, HALF), j + c, jnp.int32) for c in range(B)]
            own = (rows >= k + B) & (lanes >= k) & (lanes < k + B)
            later = lax.broadcasted_iota(jnp.int32, (B, D - n0), 1) >= j + B
            tops = [[a[pl.ds(k, 8), i * HALF : (i + 1) * HALF] for i in range(2)] for a in refs]
            bots = [[a[pl.ds(k + 8, 8), i * HALF : (i + 1) * HALF] for i in range(2)] for a in refs]
            ats = [pick(t[h], at[c]) for c in range(8) for t in tops]
            cts = [ats[n::nb] for n in range(nb)]
            ats = [pick(t[h], at[c]) for c in range(8) for t in bots]
            cbs = [ats[n::nb] for n in range(nb)]
            pts = [jnp.ones((8, HALF), F32) for _ in range(nb)]
            pbs = [jnp.ones((8, HALF), F32) for _ in range(nb)]
            for n in range(nb):
                tops[n][h] = jnp.where(first, unit, tops[n][h])
                bots[n][h] = jnp.where(first, 0.0, bots[n][h])
            for r in range(8):
                for n in range(nb):
                    top, bot, ct, cb = tops[n], bots[n], cts[n], cbs[n]
                    piv = row_of(ct[r], r)
                    inv = 1.0 / piv
                    pts[n] = jnp.where(row == r, piv, pts[n])
                    lt = jnp.where(row > r, ct[r] * inv, 0.0)
                    lb = cb[r] * inv
                    for c in range(r + 1, 8):
                        u = row_of(ct[c], r)
                        ct[c] = ct[c] - lt * u
                        cb[c] = cb[c] - lb * u
                    for i in range(2):
                        u = row_of(top[i], r)
                        if r < 7:
                            top[i] = top[i] - lt * u
                        bot[i] = bot[i] - lb * u
            ats = [pick(t[h], at[8 + c]) for c in range(8) for t in bots]
            cts = [ats[n::nb] for n in range(nb)]
            for n in range(nb):
                tops[n][h] = jnp.where(second, 0.0, tops[n][h])
                bots[n][h] = jnp.where(second, unit2, bots[n][h])
            for r in range(8):
                for n in range(nb):
                    bot, ct = bots[n], cts[n]
                    piv = row_of(ct[r], r)
                    pbs[n] = jnp.where(row == r, piv, pbs[n])
                    if r == 7:
                        continue
                    lb = jnp.where(row > r, ct[r] * (1.0 / piv), 0.0)
                    for c in range(r + 1, 8):
                        ct[c] = ct[c] - lb * row_of(ct[c], r)
                    for i in range(2):
                        bot[i] = bot[i] - lb * row_of(bot[i], r)
            scaled = []
            for n in range(nb):
                rt = lax.rsqrt(pts[n])
                rb = lax.rsqrt(pbs[n])
                scaled.append(
                    jnp.concatenate(
                        [
                            jnp.concatenate([tops[n][0] * rt, tops[n][1] * rt], 1),
                            jnp.concatenate([bots[n][0] * rb, bots[n][1] * rb], 1),
                        ],
                        0,
                    )
                )
            updates = []
            for n in range(nb):
                hi, md, lo = split3(scaled[n])
                right = jnp.concatenate([hi, lo, md, hi, md, hi], 0)
                hi, md, lo = split3(jnp.where(later, scaled[n][:, n0:], 0.0))
                left = jnp.concatenate([lo, hi, md, md, hi, hi], 0)
                updates.append(dg(left, right, 0, 0))
            for n in range(nb):
                for i in range(2):
                    old = refs[n][n0:, i * HALF : (i + 1) * HALF]
                    kept = jnp.where(own, 0.0, old) if i == h else old
                    refs[n][n0:, i * HALF : (i + 1) * HALF] = (
                        kept - updates[n][:, i * HALF : (i + 1) * HALF]
                    )
                refs[n][pl.ds(k, B), :] = scaled[n]
            return carry

        lax.fori_loop(0, HALF // B, panel, 0)


TABLE = (
    (6, 1, 3, 8, 0, 0, 2, 7, 7, 9),
    (5, 4, 0, 0, 0, 0, 1, 2, 6, 8),
    (4, 5, 3, 6, 0, 0, 2, 5, 9, 8),
    (6, 3, 1, 8, 2, 5, 3, 10, 8, 9),
)


def eye_value():
    r, c = square_iota()
    return jnp.where(r == c, 1.0, 0.0)


def pair_kernel(pos_ref, c_ref, r0, r1, w_ref, v_ref, buf):
    x = pos_ref[1]
    odd = lax.rem(x, 2)
    high = x // 2
    buf[odd] = c_ref[0]
    buf[1 - odd] = r0[...]
    buf[2 + high] = c_ref[1]
    buf[3 - high] = r1[...]
    w = mm(buf[1], buf[0])
    v = mm(buf[3], buf[2])
    outer = (x == 0) | (x == 3)
    w_ref[...] = w
    v_ref[...] = jnp.where(outer, buf[2], v)


def window_kernel(tab_ref, c_ref, r0, r1, w, q0, q1, prev_ref, t_ref, buf):
    buf[0] = c_ref[0]
    buf[1] = c_ref[1]
    for k, ref in enumerate((r0, r1, w, q0, q1)):
        buf[2 + k] = ref[...]
    buf[7] = eye_value()

    def step(i, _):
        buf[8 + i] = mm(buf[tab_ref[2 * i]], buf[tab_ref[2 * i + 1]])
        return 0

    lax.fori_loop(0, tab_ref[6], step, 0)
    prev_ref[0] = buf[tab_ref[7]]
    prev_ref[1] = buf[tab_ref[8]]
    t_ref[...] = buf[tab_ref[9]]


def entry_kernel(pos_ref, t1, t2, t3, e_ref, buf):
    z = pos_ref[0]
    buf[0] = eye_value()
    for k, ref in enumerate((t1, t2, t3)):
        buf[1 + k] = ref[...]
    e_ref[...] = buf[z]

    def step(i, _):
        e_ref[...] = mm(buf[z - 1 - i], e_ref[...])
        return 0

    lax.fori_loop(0, z - 1, step, 0)


def refinement(y, passes):
    r, c = square_iota()
    err = mm(y, y, 0, 0, passes=3) - jnp.where(r == c, 1.0, 0.0)
    upper = jnp.where(c > r, err, jnp.where(c == r, 0.5 * err, 0.0))
    return mm(y, upper, passes=passes), err


def total_of(value):
    return jnp.sum(jnp.sum(value, axis=0, keepdims=True), axis=1, keepdims=True)


def head_kernel(pos_ref, prev_ref, own, c_ref, head_ref, gram_ref):
    mine = pos_ref[2]
    before = mm(prev_ref[mine], own[...])
    after = mm(c_ref[mine], before)
    head_ref[0] = before
    head_ref[1] = after
    gram_ref[0] = mm(before, before, 0, 0, passes=GRAM)
    gram_ref[1] = mm(after, after, 0, 0, passes=GRAM)


def solve_kernel(
    pos_ref,
    prev_ref,
    head_ref,
    gram_ref,
    other,
    c_ref,
    d_ref,
    bound_ref,
    n_ref,
    r_ref,
    before_ref,
    trips_ref,
    whole_ref,
    *scratch,
):
    refs, m_ref, now = scratch[:4], scratch[4], scratch[5]
    slots = (pos_ref[2], 1 - pos_ref[2])
    rest = slots[1]
    before = mm(prev_ref[rest], other[...])
    after = mm(c_ref[rest], before)
    m_ref[0, 0] = head_ref[0]
    m_ref[1, 0] = head_ref[1]
    m_ref[0, 1] = before
    m_ref[1, 1] = after
    refs[0][...] = gram_ref[0]
    refs[2][...] = gram_ref[1]
    refs[1][...] = mm(before, before, 0, 0, passes=GRAM)
    refs[3][...] = mm(after, after, 0, 0, passes=GRAM)
    for n, m in enumerate(slots):
        before_ref[m] = m_ref[0, n]
    chol_inv(refs)
    r, c = square_iota()

    def factors(t, worst):
        inv = [
            jnp.where(c <= r, jnp.where(t == 0, refs[m][...], refs[2 + m][...]), 0.0)
            for m in range(2)
        ]
        ys = [mm(m_ref[t, m], inv[m], 1, 1) for m in range(2)]
        for m in range(2):
            change, err = refinement(ys[m], 1)
            m_ref[t, m] = ys[m] - change
            worst = jnp.maximum(worst, jnp.where(total_of(err * err) < ORTHO2, 0.0, 1.0))
        return worst

    worst = lax.fori_loop(0, 2, factors, jnp.zeros((1, 1), F32))
    fine = bound_of(bound_ref[...]) < LIMIT
    trips_ref[0] = jnp.where(fine, jnp.where(worst[0, 0] > 0.0, 1, 0), 16)
    whole_ref[0] = jnp.where(fine, 0, 1)

    def results(t, carry):
        left = [jnp.where(t == 0, c_ref[m], d_ref[m]) for m in slots]
        part = [mm(left[m], m_ref[t, m], passes=SOLVE) for m in range(2)]
        out = [mm(m_ref[1, m], part[m], 0, 0, passes=SOLVE) for m in range(2)]
        for m in range(2):
            now[m] = out[m]

        @pl.when(t == 0)
        def _():
            for n, m in enumerate(slots):
                r_ref[m] = jnp.where(c >= r, now[n], 0.0)

        @pl.when(t == 1)
        def _():
            for n, m in enumerate(slots):
                n_ref[m] = now[n]

        return carry

    lax.fori_loop(0, 2, results, 0)


def gauge_kernel(pos_ref, prev_ref, c_ref, out_ref, g_ref, b_ref):
    eye = eye_value()
    row = lax.broadcasted_iota(jnp.int32, (8, HALF), 0)
    lane = lax.broadcasted_iota(jnp.int32, (8, HALF), 1)
    norms = []
    for m in range(2):
        full = mm(c_ref[m], prev_ref[m], passes=3)
        gram = mm(full, full, 0, 0, passes=3)
        norm = jnp.sqrt(total_of(gram * gram))
        g_ref[m] = gram / norm
    for m in range(2):
        b_ref[m] = mm(g_ref[m], g_ref[m], passes=3)
    for _ in range(3):
        for m in range(2):
            b_ref[m] = mm(b_ref[m], b_ref[m], passes=1)
    for m in range(2):
        top = jnp.exp(0.0625 * 0.5 * jnp.log(total_of(b_ref[m] * b_ref[m]))) * 1.02
        b_ref[m] = eye - g_ref[m] / top
    for t in range(10):
        for m in range(2):
            b_ref[m] = mm(b_ref[m], b_ref[m], passes=3 if t < 3 else 1)
    out = jnp.zeros((8, HALF), F32)
    for m in range(2):
        norm = jnp.maximum(total_of(b_ref[m] * b_ref[m]), 1.0e-30)
        low = jnp.maximum(1.0 - jnp.exp(jnp.log(norm) / 2048.0), 1.0e-9)
        value = jnp.broadcast_to(-jnp.log(low), (8, HALF))
        out = jnp.where((row == m) & (lane == pos_ref[3]), value, out)
    out_ref[...] = out


def bound_of(v):
    lane = lax.broadcasted_iota(jnp.int32, (8, HALF), 1)
    bound = v
    for z in range(3):
        whole = jnp.sum(jnp.where(lane == 4 * z + 3, v, 0.0), axis=1, keepdims=True)
        bound = bound + jnp.where(lane >= 4 * z + 4, whole, 0.0)
    bound = jnp.where(lane < 16, bound, 0.0)
    return jnp.max(jnp.max(bound, axis=0, keepdims=True), axis=1, keepdims=True)[0, 0]


def struct(*shape):
    return jax.ShapeDtypeStruct(shape, F32)


VMEM = pl.BlockSpec(memory_space=pltpu.VMEM)
SMEM = pl.BlockSpec(memory_space=pltpu.SMEM)


def call(kernel, outs, scratch, name, table=True):
    def run(*args):
        specs = [VMEM] * len(args)
        if table:
            specs[0] = SMEM
        return pl.pallas_call(
            kernel,
            out_shape=outs,
            in_specs=specs,
            out_specs=jax.tree.map(lambda o: SMEM if o.dtype == jnp.int32 else VMEM, outs),
            scratch_shapes=[pltpu.VMEM(shape, F32) for shape in scratch],
            compiler_params=pltpu.CompilerParams(vmem_limit_bytes=48 * 2**20),
            name=name,
        )(*args)

    return run


SQUARE = struct(D, D)
TWO = struct(2, D, D)
TILE = struct(8, HALF)
COUNT = jax.ShapeDtypeStruct((1,), jnp.int32)
pair = call(pair_kernel, (SQUARE, SQUARE), [(4, D, D)], "pair")
window = call(window_kernel, (TWO, SQUARE), [(11, D, D)], "window")
entry = call(entry_kernel, SQUARE, [(4, D, D)], "entry")
solve = call(
    solve_kernel,
    (TWO, TWO, TWO, COUNT, COUNT),
    [(D, D)] * 4 + [(2, 2, D, D), (2, D, D)],
    "solve",
)
head = call(head_kernel, (TWO, TWO), [], "head")
gauge = call(gauge_kernel, TILE, [(2, D, D), (2, D, D)], "gauge")


highest = lax.Precision.HIGHEST


def product(left, right):
    return jnp.matmul(left, right, precision=highest, preferred_element_type=F32)


def flip(value):
    return jnp.swapaxes(value, -1, -2)


def orthonormal(panel):
    def turn(t, y):
        gram = product(flip(y), y)
        mean = jnp.trace(gram, axis1=-2, axis2=-1)[:, None, None] / D
        gram = gram + jnp.where(t == 0, 1.0e-5, 0.0) * mean * jnp.eye(D, dtype=F32)
        lower = jnp.linalg.cholesky(gram)
        return flip(lax.linalg.triangular_solve(lower, flip(y), left_side=True, lower=True))

    return lax.fori_loop(0, 3, turn, panel)


def one_block(before, coupling, diagonal):
    def half(t, carried):
        panel, q = carried
        panel = jnp.where(t == 0, panel, product(coupling, q))
        return panel, orthonormal(panel)

    panel, q = lax.fori_loop(0, 2, half, (before, before))
    new = product(product(flip(q), diagonal), q)
    return new, jnp.triu(product(flip(q), panel)), q


def x_move(value, to):
    return lax.ppermute(value, "row", [(i, (i // 4) * 4 + to(i % 4)) for i in range(16)])


def z_move(value, s):
    return lax.ppermute(value, "row", [(i, i + 4 * s) for i in range(16 - 4 * s)])


def z_ring(value, s):
    return lax.ppermute(value, "row", [(i, (i + 4 * s) % 16) for i in range(16)])


def x_pairs(value):
    return x_move(value, lambda x: x ^ 1)


def x_mirror(value):
    return x_move(value, lambda x: 3 - x)


def largest(value, moves):
    return functools.reduce(jnp.maximum, moves, value)


def shards(diag_blocks, coupling_blocks):
    diagonal = diag_blocks.reshape(2, D, D)
    coupling = coupling_blocks.reshape(2, D, D)
    position = lax.axis_index("row")
    z, x = position // 4, position % 4
    mine = jnp.where((x == 0) | (x == 3), 1, 0)
    pos = jnp.stack([z, x, mine, position]).astype(jnp.int32)
    table = jnp.asarray(TABLE, jnp.int32)[x]

    r0, r1 = x_pairs(coupling[0]), x_mirror(coupling[1])
    w, v = pair(pos, coupling, r0, r1)
    q0, q1 = x_mirror(w), x_pairs(v)
    prev, total = window(table, coupling, r0, r1, w, q0, q1)
    below = [z_move(total, s) for s in (1, 2, 3)]
    gauged = gauge(pos, prev, coupling)
    gauged = largest(gauged, [x_move(gauged, lambda x, s=s: (x + s) % 4) for s in (1, 2, 3)])
    gauged, *below = lax.optimization_barrier((gauged, *below))
    own = entry(pos, *below)
    gauged, own = lax.optimization_barrier((gauged, own))
    other = x_pairs(own)
    bound = largest(gauged, [z_ring(gauged, s) for s in (1, 2, 3)])
    new, tri, before, trips, whole = solve(
        pos, prev, *head(pos, prev, own, coupling), other, coupling, diagonal, bound
    )
    whole = whole.reshape(()) > 0

    def step(i, carried):
        q, new, tri = carried
        q = jnp.where(whole & (i == 0), jnp.eye(D, dtype=F32), q)
        new_now, tri_now, q = one_block(q, coupling, diagonal)
        keep = (i == position) | jnp.logical_not(whole)
        new = jnp.where(keep, new_now, new)
        tri = jnp.where(keep, tri_now, tri)
        q = lax.cond(
            whole,
            lambda q: lax.ppermute(q, "row", [(j, j + 1) for j in range(15)]),
            lambda q: q,
            q,
        )
        return q, new, tri

    _, new, tri = lax.fori_loop(0, trips.reshape(()), step, (before, new, tri))
    shape = diag_blocks.shape
    return new.reshape(shape), tri.reshape(shape)


def solution(mesh):
    placed = P("section", None, "row", None, None)
    return jax.shard_map(
        shards,
        mesh=mesh,
        in_specs=(placed, placed),
        out_specs=(placed, placed),
        check_vma=False,
    )
```
